512 devices in a mesh: dp: 16 (over z, core), fsdp: 32 (over x, y).
Axes of the slice: x: 4, y: 8, z: 8, core: 2. Of those that a mesh axis runs over, the one named last changes fastest.
Arguments:
- replica_grads: bfloat16 [16, 8192, 4096], P('dp', 'fsdp'), may hold values from -4 to 4
- slot_table: int32 [32], replicated, may hold values from 0 to 63, as said below
- left_gram_state: float32 [64, 4, 16, 16, 1024], P('fsdp', None, 'dp')
- right_gram_state: float32 [64, 4, 16, 16, 1024], P('fsdp', None, 'dp')
- left_inverse_root: bfloat16 [64, 4, 16, 16, 1024], P('fsdp', None, 'dp')
- right_inverse_root: bfloat16 [64, 4, 16, 16, 1024], P('fsdp', None, 'dp')
Outputs:
- direction: bfloat16 [32, 16, 16, 4096], P('fsdp', 'dp')
- left_new: float32 [64, 4, 16, 16, 1024], P('fsdp', None, 'dp')
- right_new: float32 [64, 4, 16, 16, 1024], P('fsdp', None, 'dp')
The draws below stay inside these ranges and needn't reach their ends.
Inputs may be any that keep to these rules, and one draw needn't show every extreme that they name: `slot_table`: the entries are distinct; slot v belongs to owner v // 2 of the flat shards' devices; some owner holds 2 blocks.
All inputs are finite; a program needn't handle non-finite values.
Results may differ from the reference program's by a relative error of at most 0.02.
Values may be sent and summed in bfloat16 or wider, within the bound.
No kernel may reach another device: no remote copies, remote signals or barrier semaphores. Data moves between devices by JAX's collectives and lax.ppermute only.
A program may use at most 128 MiB of HBM per device.

```python
import math
import jax
import jax.numpy as jnp
from jax import lax

D = 4096
BLOCK_ORDER = 1024
LAYERS = 2
NBLK = 32
STRIP_ROWS = 16
SHARDS_PER_ROW = 4
OWNER_SLOTS = 2
SLOT_TOTAL = 64
BANDS = 32
SHARD_STRIPS = 16
N_DP = 16


def symmetric_draw(key, diagonal_lower, diagonal_upper, spread):
    jitter_key, diagonal_key = jax.random.split(key)
    jitter_portion = jax.random.normal(jitter_key, (SLOT_TOTAL, BLOCK_ORDER, BLOCK_ORDER), jnp.float32)
    diagonal_values = jnp.exp(jax.random.uniform(diagonal_key, (SLOT_TOTAL, BLOCK_ORDER), jnp.float32, math.log(diagonal_lower), math.log(diagonal_upper)))
    jitter_portion = jitter_portion * (spread / math.sqrt(BLOCK_ORDER))
    symmetric = (jitter_portion + jnp.swapaxes(jitter_portion, 1, 2)) * 0.70710678
    square_matrix = symmetric + jnp.eye(BLOCK_ORDER, dtype=jnp.float32)[None] * diagonal_values[:, :, None]
    return square_matrix.reshape(SLOT_TOTAL, SHARDS_PER_ROW, SHARD_STRIPS, STRIP_ROWS, BLOCK_ORDER)


def draw_slot_table(key, part):
    initial_key, later_key, third_key = jax.random.split(jax.random.fold_in(key, 11), 3)
    owner_ranks = jax.random.permutation(initial_key, SLOT_TOTAL).astype(jnp.int32)
    complete_owner = jax.random.randint(later_key, (), 0, SLOT_TOTAL // OWNER_SLOTS)
    slot_indices = jnp.arange(SLOT_TOTAL, dtype=jnp.int32)
    priority = jnp.where(slot_indices // OWNER_SLOTS == complete_owner, slot_indices % OWNER_SLOTS - OWNER_SLOTS, owner_ranks)
    ordering = jnp.argsort(priority, stable=True).astype(jnp.int32)
    chosen = ordering[:NBLK]
    shuffle = jax.random.permutation(third_key, NBLK)
    return chosen[shuffle].astype(jnp.int32)


def draw_left_gram_state(key, part):
    return symmetric_draw(jax.random.fold_in(key, 1), 0.5, 2.0, 0.3)


def draw_right_gram_state(key, part):
    return symmetric_draw(jax.random.fold_in(key, 2), 0.5, 2.0, 0.3)


def draw_left_inverse_root(key, part):
    return symmetric_draw(jax.random.fold_in(key, 3), 0.6, 1.5, 0.5).astype(jnp.bfloat16)


def draw_right_inverse_root(key, part):
    return symmetric_draw(jax.random.fold_in(key, 4), 0.6, 1.5, 0.5).astype(jnp.bfloat16)


def block_scale(own_key, dims, shards, smallest, high):
    factor_of, own = 1.0, jax.random.fold_in(own_key, 6)
    for position, blocks in shards:
        steps = jnp.exp(jax.random.uniform(jax.random.fold_in(own, position), (blocks,), jnp.float32, smallest / len(shards), high / len(shards)))
        factor_of = factor_of * jnp.repeat(steps, dims[position] // blocks).reshape([-1 if axis == position else 1 for axis in range(len(dims))])
    return factor_of


def gaussian(own_key, extent, width, most, shards=(), kind=jnp.bfloat16):
    loudness = block_scale(own_key, extent, shards, -0.22, 0.18) if shards else 1.0
    array = jax.random.normal(own_key, extent, jnp.float32) * width * loudness
    return jnp.minimum(jnp.maximum(array, -most), most).astype(kind)


def setup_inputs(seed: int = 0) -> dict:
    splits = jax.random.split(jax.random.key(seed), 7)
    replica_grads = gaussian(splits[0], (N_DP, LAYERS * D, D), 0.25, 4.0, ((0, 16), (1, 32)))
    slot_table = draw_slot_table(jax.random.fold_in(splits[6], 71), 0)
    left_gram_state = draw_left_gram_state(jax.random.fold_in(splits[6], 71), 0)
    right_gram_state = draw_right_gram_state(jax.random.fold_in(splits[6], 71), 0)
    left_inverse_root = draw_left_inverse_root(jax.random.fold_in(splits[6], 71), 0)
    right_inverse_root = draw_right_inverse_root(jax.random.fold_in(splits[6], 71), 0)
    return dict(replica_grads=replica_grads, slot_table=slot_table, left_gram_state=left_gram_state, right_gram_state=right_gram_state, left_inverse_root=left_inverse_root, right_inverse_root=right_inverse_root)


def reference(replica_grads, slot_table, left_gram_state, right_gram_state, left_inverse_root, right_inverse_root):
    per_band = D // BLOCK_ORDER
    summed = jnp.sum(replica_grads.astype(jnp.float32), axis=0).astype(jnp.bfloat16)
    blocks = summed.reshape(LAYERS * per_band, BLOCK_ORDER, per_band, BLOCK_ORDER).transpose(0, 2, 1, 3).reshape(NBLK, BLOCK_ORDER, BLOCK_ORDER)
    left_factors = left_gram_state.reshape(SLOT_TOTAL, BLOCK_ORDER, BLOCK_ORDER)
    right_factors = right_gram_state.reshape(SLOT_TOTAL, BLOCK_ORDER, BLOCK_ORDER)
    left_root_stack = left_inverse_root.reshape(SLOT_TOTAL, BLOCK_ORDER, BLOCK_ORDER)
    right_root_stack = right_inverse_root.reshape(SLOT_TOTAL, BLOCK_ORDER, BLOCK_ORDER)

    def one_block(index):
        slot = slot_table[index]
        gradient = blocks[index]
        left_next = left_factors[slot] + jnp.dot(gradient, gradient.T, preferred_element_type=jnp.float32) / BLOCK_ORDER
        right_next = right_factors[slot] + jnp.dot(gradient.T, gradient, preferred_element_type=jnp.float32) / BLOCK_ORDER
        mixed_rows = jnp.dot(left_root_stack[slot], gradient, preferred_element_type=jnp.float32).astype(jnp.bfloat16)
        outcome = jnp.dot(mixed_rows, right_root_stack[slot], preferred_element_type=jnp.float32).astype(jnp.bfloat16)
        return left_next, right_next, outcome

    left_next, right_next, outcomes = lax.map(one_block, jnp.arange(NBLK, dtype=jnp.int32))
    left_new = left_factors.at[slot_table].set(left_next).reshape(left_gram_state.shape)
    right_new = right_factors.at[slot_table].set(right_next).reshape(right_gram_state.shape)
    direction = outcomes.reshape(LAYERS * per_band, per_band, BLOCK_ORDER, BLOCK_ORDER).transpose(0, 2, 1, 3)
    direction = direction.reshape(BANDS, SHARD_STRIPS, STRIP_ROWS, D)
    return direction, left_new, right_new
```

```python
import functools

import jax
import jax.numpy as jnp
from jax import lax
from jax.experimental import pallas as pl
from jax.experimental.pallas import tpu as pltpu
from jax.sharding import Mesh, PartitionSpec as P

BF = jnp.bfloat16
F32 = jnp.float32
BANDS = ("x", "yh", "yl")
ROWS = ("z", "c")
VM = pl.BlockSpec(memory_space=pltpu.VMEM)
SM = pl.BlockSpec(memory_space=pltpu.SMEM)


def call(kernel, out, inputs, scalars=0, scratch=(), flops=1000000):
    moved = sum(a.size * a.dtype.itemsize for a in inputs)
    return pl.pallas_call(
        kernel,
        out_shape=out,
        in_specs=[VM] * (len(inputs) - scalars) + [SM] * scalars,
        out_specs=jax.tree.map(lambda _: VM, out),
        scratch_shapes=scratch,
        compiler_params=pltpu.CompilerParams(vmem_limit_bytes=32 * 1024 * 1024),
        cost_estimate=pl.CostEstimate(flops=flops, bytes_accessed=moved, transcendentals=0),
    )(*inputs)


def shape(dims, dtype=BF):
    return jax.ShapeDtypeStruct(dims, dtype)


def spread_roots(left_ref, right_ref, out_ref):
    for slot in range(2):
        for sub in range(4):
            for part in range(8):
                columns = slice(part * 128, part * 128 + 128)
                out_ref[sub * 8 + part, slot, 0] = left_ref[slot, sub, 0, :, columns]
                out_ref[sub * 8 + part, slot, 1] = right_ref[slot, sub, 0, :, columns]


def pick_roots(in_ref, table_ref, out_ref):
    for block in range(32):
        out_ref[block] = in_ref[table_ref[block]]


def join_roots(in_ref, left_ref, right_ref):
    for sub in range(4):
        for part in range(8):
            columns = slice(part * 128, part * 128 + 128)
            left_ref[sub, :, columns] = in_ref[sub * 8 + part, 0]
            right_ref[sub, :, columns] = in_ref[sub * 8 + part, 1]


def add_replicas(in_ref, out_ref):
    for column in range(4):
        columns = slice(column * 1024, column * 1024 + 1024)
        total = in_ref[0, :, columns].astype(F32)
        for source in range(1, 8):
            total = total + in_ref[source, :, columns].astype(F32)
        out_ref[column] = total.astype(BF)


def place_rows(whole, mine_ref, other_ref, core):
    for z in range(8):
        for sub in range(4):
            base = sub * 256 + z * 32
            whole[pl.ds(pl.multiple_of(base + core * 16, 16), 16), :] = mine_ref[z, sub]
            whole[pl.ds(pl.multiple_of(base + 16 - core * 16, 16), 16), :] = other_ref[z, sub]


def products(mine_ref, other_ref, rows_ref, left_ref, where_ref, gram_ref, mixed_ref, whole, both):
    core = where_ref[1]
    strip = where_ref[0] * 2 + core
    place_rows(whole, mine_ref, other_ref, core)
    row = lax.broadcasted_iota(jnp.int32, (64, 1024), 0)
    column = lax.broadcasted_iota(jnp.int32, (64, 1024), 1)
    chosen = (row // 16) * 256 + strip * 16 + row % 16
    both[0:64] = rows_ref[...].reshape(64, 1024)
    both[64:128] = jnp.where(column == chosen, 1.0, 0.0).astype(BF)
    first = lax.dot_general(
        both[...], whole[...], (((1,), (1,)), ((), ())), preferred_element_type=F32
    )
    both[0:64] = first[64:128].astype(BF)
    both[64:128] = left_ref[...].reshape(64, 1024)
    second = jnp.dot(both[...], whole[...], preferred_element_type=F32)
    left_gram = (first[0:64] * (1.0 / 1024)).astype(BF)
    right_gram = (second[0:64] * (1.0 / 1024)).astype(BF)
    for sub in range(4):
        for part in range(8):
            columns = slice(part * 128, part * 128 + 128)
            gram_ref[sub * 8 + part, 0] = left_gram[sub * 16 : sub * 16 + 16, columns]
            gram_ref[sub * 8 + part, 1] = right_gram[sub * 16 : sub * 16 + 16, columns]
    mixed_ref[...] = second[64:128].astype(BF)


def to_slots(in_ref, holder_ref, out_ref):
    for slot in range(64):
        block = holder_ref[slot]
        piece = in_ref[jnp.maximum(block, 0)]
        out_ref[slot // 2, slot % 2] = jnp.where(block >= 0, piece, jnp.zeros_like(piece))


def finish_grams(in_ref, left_ref, right_ref, left_out, right_out):
    for slot in range(2):
        for sub in range(4):
            for part in range(8):
                columns = slice(part * 128, part * 128 + 128)
                piece = sub * 8 + part
                left_out[slot, sub, 0, :, columns] = left_ref[slot, sub, 0, :, columns] + in_ref[
                    piece, slot, 0
                ].astype(F32)
                right_out[slot, sub, 0, :, columns] = right_ref[slot, sub, 0, :, columns] + in_ref[
                    piece, slot, 1
                ].astype(F32)


def right_product(mine_ref, other_ref, mixed_ref, where_ref, out_ref, whole):
    place_rows(whole, mine_ref, other_ref, where_ref[1])
    out_ref[...] = (
        jnp.dot(mixed_ref[...], whole[...], preferred_element_type=F32)
        .astype(BF)
        .reshape(4, 16, 1024)
    )


def exchange(value, axes):
    return lax.all_to_all(value, axes, split_axis=0, concat_axis=0, tiled=True)


def swap(value):
    return lax.ppermute(value, "c", [(0, 1), (1, 0)])


def on_device(grads, table, left_state, right_state, left_root, right_root):
    z, core = lax.axis_index("z"), lax.axis_index("c")
    where = jnp.stack([z, core]).astype(jnp.int32)
    slots = jnp.arange(64, dtype=jnp.int32)
    blocks = jnp.arange(32, dtype=jnp.int32)
    holder = jnp.sum(jnp.where(table[None, :] == slots[:, None], blocks[None, :] + 1, 0), axis=1) - 1

    with jax.named_scope("reduce"):
        strips = grads.reshape(8, 2, 16, 4096)
        theirs = lax.dynamic_index_in_dim(strips, 1 - core, 1, keepdims=False)
        ours = lax.dynamic_index_in_dim(strips, core, 1, keepdims=False)
        pair = (ours.astype(F32) + swap(theirs).astype(F32)).astype(BF)
        arrived = exchange(pair, "z")
        strip = call(add_replicas, shape((4, 16, 1024)), [arrived])
        rows = exchange(strip, "yl")

    with jax.named_scope("roots"):
        pieces = call(spread_roots, shape((32, 2, 2, 16, 128)), [left_root, right_root])
        pieces = exchange(pieces, BANDS).reshape(64, 2, 16, 128)
        picked = call(pick_roots, shape((32, 2, 16, 128)), [pieces, table], scalars=1)
        picked = exchange(picked, BANDS)
        left_rows, right_rows = call(
            join_roots, (shape((4, 16, 1024)), shape((4, 16, 1024))), [picked]
        )

    with jax.named_scope("gather"):
        mine = exchange(jnp.broadcast_to(rows[None], (8, 4, 16, 1024)), "z")
        other = swap(mine)
        gram, mixed = call(
            products,
            (shape((32, 2, 16, 128)), shape((64, 1024))),
            [mine, other, rows, left_rows, where],
            scalars=1,
            scratch=[pltpu.VMEM((1024, 1024), BF), pltpu.VMEM((128, 1024), BF)],
            flops=2 * 256 * 1024 * 1024,
        )

    with jax.named_scope("grams"):
        gram = exchange(gram, BANDS)
        gram = call(to_slots, shape((32, 2, 2, 16, 128)), [gram, holder], scalars=1)
        gram = exchange(gram, BANDS)
        left_new, right_new = call(
            finish_grams,
            (shape(left_state.shape, F32), shape(right_state.shape, F32)),
            [gram, left_state, right_state],
        )

    with jax.named_scope("direction"):
        (right_rows, _) = lax.optimization_barrier((right_rows, mine))
        right_mine = exchange(jnp.broadcast_to(right_rows[None], (8, 4, 16, 1024)), "z")
        right_other = swap(right_mine)
        result = call(
            right_product,
            shape((4, 16, 1024)),
            [right_mine, right_other, mixed, where],
            scalars=1,
            scratch=[pltpu.VMEM((1024, 1024), BF)],
            flops=2 * 64 * 1024 * 1024,
        )
        home = exchange(result, "yl")
        direction = home.transpose(1, 0, 2).reshape(1, 1, 16, 4096)
    return direction, left_new, right_new


def solution(mesh):
    fine = Mesh(mesh.devices.reshape(8, 2, 4, 2, 4), ROWS + BANDS)
    state = P(BANDS, None, ROWS, None, None)
    return jax.shard_map(
        on_device,
        mesh=fine,
        in_specs=(P(ROWS, BANDS, None), P(), state, state, state, state),
        out_specs=(P(BANDS, ROWS, None, None), state, state),
        check_vma=False,
    )
```

```python
import jax
import jax.numpy as jnp
from jax import lax
from jax.experimental import pallas as pl
from jax.experimental.pallas import tpu as pltpu
from jax.sharding import Mesh, PartitionSpec as P


BF = jnp.bfloat16
F32 = jnp.float32
BANDS = ("x", "yh", "yl")
ROWS = ("z", "c")
DISTANCES = (4, 3, 5, 2, 6, 1, 7)
VM = pl.BlockSpec(memory_space=pltpu.VMEM)
SM = pl.BlockSpec(memory_space=pltpu.SMEM)


def call(kernel, out, inputs, scalars=0, scratch=(), flops=1000000):
    moved = sum(a.size * a.dtype.itemsize for a in inputs)
    return pl.pallas_call(
        kernel,
        out_shape=out,
        in_specs=[VM] * (len(inputs) - scalars) + [SM] * scalars,
        out_specs=jax.tree.map(lambda _: VM, out),
        scratch_shapes=scratch,
        compiler_params=pltpu.CompilerParams(vmem_limit_bytes=32 * 1024 * 1024),
        cost_estimate=pl.CostEstimate(flops=flops, bytes_accessed=moved, transcendentals=0),
    )(*inputs)


def shape(dims, dtype=BF):
    return jax.ShapeDtypeStruct(dims, dtype)


def spread_roots(left_ref, right_ref, out_ref):
    for slot in range(2):
        for sub in range(4):
            for part in range(8):
                columns = slice(part * 128, part * 128 + 128)
                out_ref[sub * 8 + part, slot, 0] = left_ref[slot, sub, 0, :, columns]
                out_ref[sub * 8 + part, slot, 1] = right_ref[slot, sub, 0, :, columns]


def pick_roots(in_ref, table_ref, out_ref):
    for block in range(32):
        out_ref[block] = in_ref[table_ref[block]]


def join_roots(in_ref, left_ref, right_ref):
    for sub in range(4):
        for part in range(8):
            columns = slice(part * 128, part * 128 + 128)
            left_ref[sub, :, columns] = in_ref[sub * 8 + part, 0]
            right_ref[sub, :, columns] = in_ref[sub * 8 + part, 1]


def pick_theirs(grads_ref, where_ref, out_ref, sems):
    copies = []
    for k in range(8):
        strip = lax.rem(where_ref[0] + k, 8) * 2 + 1 - where_ref[1]
        rows = pl.ds(pl.multiple_of(strip * 16, 16), 16)
        copies.append(pltpu.make_async_copy(grads_ref.at[0, rows, :], out_ref.at[k], sems.at[k]))
    for copy in copies:
        copy.start()
    for copy in copies:
        copy.wait()


def add_pair(grads_ref, theirs_ref, where_ref, *out_refs):
    for k in range(8):
        strip = lax.rem(where_ref[0] + k, 8) * 2 + where_ref[1]
        rows = pl.ds(pl.multiple_of(strip * 16, 16), 16)
        out_refs[k][...] = (
            grads_ref[0, rows, :].astype(F32) + theirs_ref[k].astype(F32)
        ).astype(BF)


def add_replicas(*refs):
    out_ref = refs[-1]
    for column in range(4):
        columns = slice(column * 1024, column * 1024 + 1024)
        total = refs[0][:, columns].astype(F32)
        for term in refs[1:-1]:
            total = total + term[:, columns].astype(F32)
        out_ref[column] = total.astype(BF)


def stack_rows(*refs):
    for k in range(8):
        refs[-1][k] = refs[k][...]


def place_rows(whole, mine_ref, other_ref, core, first):
    for k in range(8):
        z = lax.rem(first + 8 - k, 8)
        for sub in range(4):
            base = sub * 256 + z * 32
            whole[pl.ds(pl.multiple_of(base + core * 16, 16), 16), :] = mine_ref[k, sub]
            whole[pl.ds(pl.multiple_of(base + 16 - core * 16, 16), 16), :] = other_ref[k, sub]


def products(mine_ref, other_ref, rows_ref, left_ref, where_ref, gram_ref, mixed_ref, whole, both):
    core = where_ref[1]
    strip = where_ref[0] * 2 + core
    place_rows(whole, mine_ref, other_ref, core, where_ref[0])
    row = lax.broadcasted_iota(jnp.int32, (64, 1024), 0)
    column = lax.broadcasted_iota(jnp.int32, (64, 1024), 1)
    chosen = (row // 16) * 256 + strip * 16 + row % 16
    both[0:64] = rows_ref[...].reshape(64, 1024)
    both[64:128] = jnp.where(column == chosen, 1.0, 0.0).astype(BF)
    first = lax.dot_general(
        both[...], whole[...], (((1,), (1,)), ((), ())), preferred_element_type=F32
    )
    both[0:64] = first[64:128].astype(BF)
    both[64:128] = left_ref[...].reshape(64, 1024)
    second = jnp.dot(both[...], whole[...], preferred_element_type=F32)
    left_gram = (first[0:64] * (1.0 / 1024)).astype(BF)
    right_gram = (second[0:64] * (1.0 / 1024)).astype(BF)
    for sub in range(4):
        for part in range(8):
            columns = slice(part * 128, part * 128 + 128)
            gram_ref[sub * 8 + part, 0] = left_gram[sub * 16 : sub * 16 + 16, columns]
            gram_ref[sub * 8 + part, 1] = right_gram[sub * 16 : sub * 16 + 16, columns]
    mixed_ref[...] = second[64:128].astype(BF)


def to_slots(in_ref, holder_ref, out_ref):
    for slot in range(64):
        block = holder_ref[slot]
        piece = in_ref[jnp.maximum(block, 0)]
        out_ref[slot // 2, slot % 2] = jnp.where(block >= 0, piece, jnp.zeros_like(piece))


def finish_grams(in_ref, left_ref, right_ref, left_out, right_out):
    for slot in range(2):
        for sub in range(4):
            for part in range(8):
                columns = slice(part * 128, part * 128 + 128)
                piece = sub * 8 + part
                left_out[slot, sub, 0, :, columns] = left_ref[slot, sub, 0, :, columns] + in_ref[
                    piece, slot, 0
                ].astype(F32)
                right_out[slot, sub, 0, :, columns] = right_ref[slot, sub, 0, :, columns] + in_ref[
                    piece, slot, 1
                ].astype(F32)


def right_product(mine_ref, other_ref, mixed_ref, where_ref, *refs):
    whole, rows = refs[4:]
    place_rows(whole, mine_ref, other_ref, where_ref[1], where_ref[0])
    product = jnp.dot(mixed_ref[...], whole[...], preferred_element_type=F32)
    rows[...] = product.astype(BF).reshape(4, 16, 1024)
    for k in range(4):
        refs[k][...] = rows[lax.rem(where_ref[2] + k, 4)]


def join_columns(*refs):
    where_ref, out_ref = refs[4:]
    for k in range(4):
        column = lax.rem(where_ref[2] + 4 - k, 4) * 1024
        out_ref[0, 0, :, pl.ds(pl.multiple_of(column, 1024), 1024)] = refs[k][...]


def exchange(value, axes):
    return lax.all_to_all(value, axes, split_axis=0, concat_axis=0, tiled=True)


def swap(value):
    return lax.ppermute(value, "c", [(0, 1), (1, 0)])


def shift(value, axis, distance):
    size = lax.axis_size(axis)
    return lax.ppermute(value, axis, [(i, (i + distance) % size) for i in range(size)])


def gathered(rows):
    arrived = {k: shift(rows, "z", k) for k in DISTANCES}
    arrived[0] = rows
    return call(stack_rows, shape((8, 4, 16, 1024)), [arrived[k] for k in range(8)])


def step(grads, table, left_state, right_state, left_root, right_root):
    z, core = lax.axis_index("z"), lax.axis_index("c")
    where = jnp.stack([z, core, lax.axis_index("yl")]).astype(jnp.int32)
    slots = jnp.arange(64, dtype=jnp.int32)
    blocks = jnp.arange(32, dtype=jnp.int32)
    holder = jnp.sum(jnp.where(table[None, :] == slots[:, None], blocks[None, :] + 1, 0), axis=1) - 1

    theirs = pl.pallas_call(
        pick_theirs,
        out_shape=shape((8, 16, 4096)),
        in_specs=[pl.BlockSpec(memory_space=pltpu.HBM), SM],
        out_specs=VM,
        scratch_shapes=[pltpu.SemaphoreType.DMA((8,))],
        cost_estimate=pl.CostEstimate(flops=1000000, bytes_accessed=2097152, transcendentals=0),
    )(grads, where)
    pairs = call(
        add_pair, (shape((16, 4096)),) * 8, [grads, swap(theirs), where], scalars=1
    )
    terms = [pairs[0]] + [shift(pairs[k], "z", k) for k in DISTANCES]
    strip = call(add_replicas, shape((4, 16, 1024)), terms)
    rows = exchange(strip, "yl")

    pieces = call(spread_roots, shape((32, 2, 2, 16, 128)), [left_root, right_root])
    pieces = exchange(pieces, BANDS).reshape(64, 2, 16, 128)
    picked = call(pick_roots, shape((32, 2, 16, 128)), [pieces, table], scalars=1)
    picked, rows = lax.optimization_barrier((picked, rows))
    picked = exchange(picked, BANDS)
    left_rows, right_rows = call(join_roots, (shape((4, 16, 1024)), shape((4, 16, 1024))), [picked])

    mine = gathered(rows)
    other = swap(mine)
    gram, mixed = call(
        products,
        (shape((32, 2, 16, 128)), shape((64, 1024))),
        [mine, other, rows, left_rows, where],
        scalars=1,
        scratch=[pltpu.VMEM((1024, 1024), BF), pltpu.VMEM((128, 1024), BF)],
        flops=2 * 256 * 1024 * 1024,
    )

    gram = exchange(gram, BANDS)
    gram = call(to_slots, shape((32, 2, 2, 16, 128)), [gram, holder], scalars=1)
    gram = exchange(gram, BANDS)
    left_new, right_new = call(
        finish_grams,
        (shape(left_state.shape, F32), shape(right_state.shape, F32)),
        [gram, left_state, right_state],
    )

    right_rows, mixed = lax.optimization_barrier((right_rows, mixed))
    right_mine = gathered(right_rows)
    right_other = swap(right_mine)
    result = call(
        right_product,
        (shape((16, 1024)),) * 4,
        [right_mine, right_other, mixed, where],
        scalars=1,
        scratch=[pltpu.VMEM((1024, 1024), BF), pltpu.VMEM((4, 16, 1024), BF)],
        flops=2 * 64 * 1024 * 1024,
    )
    home = [result[0]] + [shift(result[k], "yl", k) for k in range(1, 4)]
    direction = call(join_columns, shape((1, 1, 16, 4096)), [*home, where], scalars=1)
    return direction, left_new, right_new


def solution(mesh):
    fine = Mesh(mesh.devices.reshape(8, 2, 4, 2, 4), ROWS + BANDS)
    state = P(BANDS, None, ROWS, None, None)
    return jax.shard_map(
        step,
        mesh=fine,
        in_specs=(P(ROWS, BANDS, None), P(), state, state, state, state),
        out_specs=(P(BANDS, ROWS, None, None), state, state),
        check_vma=False,
    )
```

```python
import jax
import jax.numpy as jnp
from jax import lax
from jax.experimental import pallas as pl
from jax.experimental.pallas import tpu as pltpu
from jax.sharding import Mesh, PartitionSpec as P


BF = jnp.bfloat16
F32 = jnp.float32
BANDS = ("x", "yh", "yl")
ROWS = ("z", "c")
DISTANCES = (4, 3, 5, 2, 6, 1, 7)
VM = pl.BlockSpec(memory_space=pltpu.VMEM)
SM = pl.BlockSpec(memory_space=pltpu.SMEM)


def call(kernel, out, inputs, scalars=0, scratch=(), flops=1000000):
    moved = sum(a.size * a.dtype.itemsize for a in inputs)
    return pl.pallas_call(
        kernel,
        out_shape=out,
        in_specs=[VM] * (len(inputs) - scalars) + [SM] * scalars,
        out_specs=jax.tree.map(lambda _: VM, out),
        scratch_shapes=scratch,
        compiler_params=pltpu.CompilerParams(vmem_limit_bytes=32 * 1024 * 1024),
        cost_estimate=pl.CostEstimate(flops=flops, bytes_accessed=moved, transcendentals=0),
    )(*inputs)


def shape(dims, dtype=BF):
    return jax.ShapeDtypeStruct(dims, dtype)


def spread_roots(left_ref, right_ref, out_ref):
    for slot in range(2):
        for sub in range(4):
            for part in range(8):
                columns = slice(part * 128, part * 128 + 128)
                out_ref[sub * 8 + part, slot, 0] = left_ref[slot, sub, 0, :, columns]
                out_ref[sub * 8 + part, slot, 1] = right_ref[slot, sub, 0, :, columns]


def pick_roots(in_ref, table_ref, out_ref):
    for block in range(32):
        out_ref[block] = in_ref[table_ref[block]]


def join_roots(in_ref, left_ref, right_ref):
    for sub in range(4):
        for part in range(8):
            columns = slice(part * 128, part * 128 + 128)
            left_ref[sub, :, columns] = in_ref[sub * 8 + part, 0]
            right_ref[sub, :, columns] = in_ref[sub * 8 + part, 1]


def add_pair(grads_ref, theirs_ref, where_ref, *out_refs):
    for k in range(8):
        strip = lax.rem(where_ref[0] + k, 8) * 2 + where_ref[1]
        rows = pl.ds(pl.multiple_of(strip * 16, 16), 16)
        out_refs[k][...] = (
            grads_ref[0, rows, :].astype(F32) + theirs_ref[0, rows, :].astype(F32)
        ).astype(BF)


def add_replicas(*refs):
    out_ref = refs[-1]
    for column in range(4):
        columns = slice(column * 1024, column * 1024 + 1024)
        total = refs[0][:, columns].astype(F32)
        for term in refs[1:-1]:
            total = total + term[:, columns].astype(F32)
        total = total.astype(BF)
        for z in range(8):
            out_ref[z * 4 + column] = total


def place(whole, rows, z, parity):
    for sub in range(4):
        base = sub * 256 + z * 32 + parity * 16
        whole[pl.ds(pl.multiple_of(base, 16), 16), :] = rows[sub]


def products(mine_ref, other_ref, left_ref, where_ref, gram_ref, mixed_ref, whole, both):
    core = where_ref[1]
    strip = where_ref[0] * 2 + core
    for z in range(8):
        place(whole, mine_ref.at[z], z, core)
        place(whole, other_ref.at[z], z, 1 - core)
    row = lax.broadcasted_iota(jnp.int32, (64, 1024), 0)
    column = lax.broadcasted_iota(jnp.int32, (64, 1024), 1)
    chosen = (row // 16) * 256 + strip * 16 + row % 16
    both[0:64] = mine_ref[where_ref[0]].reshape(64, 1024)
    both[64:128] = jnp.where(column == chosen, 1.0, 0.0).astype(BF)
    first = lax.dot_general(
        both[...], whole[...], (((1,), (1,)), ((), ())), preferred_element_type=F32
    )
    both[0:64] = first[64:128].astype(BF)
    both[64:128] = left_ref[...].reshape(64, 1024)
    second = jnp.dot(both[...], whole[...], preferred_element_type=F32)
    left_gram = (first[0:64] * (1.0 / 1024)).astype(BF)
    right_gram = (second[0:64] * (1.0 / 1024)).astype(BF)
    for sub in range(4):
        for part in range(8):
            columns = slice(part * 128, part * 128 + 128)
            gram_ref[sub * 8 + part, 0] = left_gram[sub * 16 : sub * 16 + 16, columns]
            gram_ref[sub * 8 + part, 1] = right_gram[sub * 16 : sub * 16 + 16, columns]
    mixed_ref[...] = second[64:128].astype(BF)


def to_slots(in_ref, holder_ref, out_ref):
    for slot in range(64):
        block = holder_ref[slot]
        piece = in_ref[jnp.maximum(block, 0)]
        out_ref[slot // 2, slot % 2] = jnp.where(block >= 0, piece, jnp.zeros_like(piece))


def finish_grams(in_ref, left_ref, right_ref, left_out, right_out):
    for slot in range(2):
        for sub in range(4):
            for part in range(8):
                columns = slice(part * 128, part * 128 + 128)
                piece = sub * 8 + part
                left_out[slot, sub, 0, :, columns] = left_ref[slot, sub, 0, :, columns] + in_ref[
                    piece, slot, 0
                ].astype(F32)
                right_out[slot, sub, 0, :, columns] = right_ref[slot, sub, 0, :, columns] + in_ref[
                    piece, slot, 1
                ].astype(F32)


def pair_up(mine_ref, other_ref, where_ref, out_ref):
    out_ref[where_ref[1]] = mine_ref[...]
    out_ref[1 - where_ref[1]] = other_ref[...]


def take_parity(in_ref, where_ref, out_ref):
    out_ref[...] = in_ref[where_ref[1]]


def stack_rows(first_ref, second_ref, third_ref, last_ref, out_ref):
    for hop, ref in enumerate((first_ref, second_ref, third_ref)):
        out_ref[2 * hop] = ref[0]
        out_ref[2 * hop + 1] = ref[1]
    out_ref[6] = last_ref[...]


def right_product(pair_ref, mine_ref, other_ref, mixed_ref, where_ref, *refs):
    whole, rows = refs[4:]
    z, core = where_ref[0], where_ref[1]
    for parity in range(2):
        place(whole, pair_ref.at[parity], z, parity)
        for hop in range(3):
            ahead = (1 - 2 * core) * (hop + 1)
            place(whole, mine_ref.at[2 * hop + parity], lax.rem(z + 8 + ahead, 8), parity)
            place(whole, other_ref.at[2 * hop + parity], lax.rem(z + 8 - ahead, 8), parity)
    place(whole, mine_ref.at[6], lax.rem(z + 4, 8), core)
    place(whole, other_ref.at[6], lax.rem(z + 4, 8), 1 - core)
    product = jnp.dot(mixed_ref[...], whole[...], preferred_element_type=F32)
    rows[...] = product.astype(BF).reshape(4, 16, 1024)
    for k in range(4):
        refs[k][...] = rows[lax.rem(where_ref[2] + k, 4)]


def join_columns(*refs):
    where_ref, out_ref = refs[4:]
    for k in range(4):
        column = lax.rem(where_ref[2] + 4 - k, 4) * 1024
        out_ref[0, 0, :, pl.ds(pl.multiple_of(column, 1024), 1024)] = refs[k][...]


def exchange(value, axes):
    return lax.all_to_all(value, axes, split_axis=0, concat_axis=0, tiled=True)


def swap(value):
    return lax.ppermute(value, "c", [(0, 1), (1, 0)])


def shift(value, axis, distance):
    size = lax.axis_size(axis)
    return lax.ppermute(value, axis, [(i, (i + distance) % size) for i in range(size)])


def around(value):
    pairs = [(2 * z + c, 2 * ((z - 1 + 2 * c) % 8) + c) for z in range(8) for c in range(2)]
    return lax.ppermute(value, ROWS, pairs)


def step(grads, table, left_state, right_state, left_root, right_root):
    z, core = lax.axis_index("z"), lax.axis_index("c")
    where = jnp.stack([z, core, lax.axis_index("yl")]).astype(jnp.int32)
    slots = jnp.arange(64, dtype=jnp.int32)
    blocks = jnp.arange(32, dtype=jnp.int32)
    holder = jnp.sum(jnp.where(table[None, :] == slots[:, None], blocks[None, :] + 1, 0), axis=1) - 1

    theirs = swap(grads)
    pairs = call(add_pair, (shape((16, 4096)),) * 8, [grads, theirs, where], scalars=1)
    terms = [pairs[0]] + [shift(pairs[k], "z", k) for k in DISTANCES]
    strip = call(add_replicas, shape((32, 16, 1024)), terms)

    pieces = call(spread_roots, shape((32, 2, 2, 16, 128)), [left_root, right_root])
    pieces = exchange(pieces, BANDS).reshape(64, 2, 16, 128)
    picked = call(pick_roots, shape((32, 2, 16, 128)), [pieces, table], scalars=1)
    picked = exchange(picked, BANDS)
    left_rows, right_rows = call(join_roots, (shape((4, 16, 1024)), shape((4, 16, 1024))), [picked])

    mine = exchange(strip, ("z", "yl")).reshape(8, 4, 16, 1024)
    other = swap(mine)
    gram, mixed = call(
        products,
        (shape((32, 2, 16, 128)), shape((64, 1024))),
        [mine, other, left_rows, where],
        scalars=1,
        scratch=[pltpu.VMEM((1024, 1024), BF), pltpu.VMEM((128, 1024), BF)],
        flops=2 * 256 * 1024 * 1024,
    )

    gram = exchange(gram, BANDS)
    gram = call(to_slots, shape((32, 2, 2, 16, 128)), [gram, holder], scalars=1)
    gram = exchange(gram, BANDS)
    left_new, right_new = call(
        finish_grams,
        (shape(left_state.shape, F32), shape(right_state.shape, F32)),
        [gram, left_state, right_state],
    )

    theirs = swap(right_rows)
    pair = call(
        pair_up, shape((2, 4, 16, 1024)), [right_rows, theirs, where], scalars=1
    )
    rings = [around(pair)]
    rings.append(around(rings[0]))
    rings.append(around(rings[1]))
    half = call(take_parity, shape((4, 16, 1024)), [rings[2], where], scalars=1)
    rings.append(around(half))
    right_mine = call(stack_rows, shape((7, 4, 16, 1024)), rings)
    right_other = swap(right_mine)
    result = call(
        right_product,
        (shape((16, 1024)),) * 4,
        [pair, right_mine, right_other, mixed, where],
        scalars=1,
        scratch=[pltpu.VMEM((1024, 1024), BF), pltpu.VMEM((4, 16, 1024), BF)],
        flops=2 * 64 * 1024 * 1024,
    )
    home = [result[0]] + [shift(result[k], "yl", k) for k in range(1, 4)]
    direction = call(join_columns, shape((1, 1, 16, 4096)), [*home, where], scalars=1)
    return direction, left_new, right_new


def solution(mesh):
    fine = Mesh(mesh.devices.reshape(8, 2, 4, 2, 4), ROWS + BANDS)
    state = P(BANDS, None, ROWS, None, None)
    return jax.shard_map(
        step,
        mesh=fine,
        in_specs=(P(ROWS, BANDS, None), P(), state, state, state, state),
        out_specs=(P(BANDS, ROWS, None, None), state, state),
        check_vma=False,
    )
```

```python
import jax
import jax.numpy as jnp
from jax import lax
from jax.experimental import pallas as pl
from jax.experimental.pallas import tpu as pltpu
from jax.sharding import Mesh, PartitionSpec as P


BF = jnp.bfloat16
F32 = jnp.float32
BANDS = ("x", "yh", "yl")
ROWS = ("z", "c")
VM = pl.BlockSpec(memory_space=pltpu.VMEM)
SM = pl.BlockSpec(memory_space=pltpu.SMEM)


def call(kernel, out, inputs, scalars=0, scratch=(), flops=1000000):
    moved = sum(a.size * a.dtype.itemsize for a in inputs)
    return pl.pallas_call(
        kernel,
        out_shape=out,
        in_specs=[VM] * (len(inputs) - scalars) + [SM] * scalars,
        out_specs=jax.tree.map(lambda _: VM, out),
        scratch_shapes=scratch,
        compiler_params=pltpu.CompilerParams(vmem_limit_bytes=32 * 1024 * 1024),
        cost_estimate=pl.CostEstimate(flops=flops, bytes_accessed=moved, transcendentals=0),
    )(*inputs)


def shape(dims, dtype=BF):
    return jax.ShapeDtypeStruct(dims, dtype)


def spread_roots(left_ref, right_ref, out_ref):
    for slot in range(2):
        for sub in range(4):
            for part in range(8):
                columns = slice(part * 128, part * 128 + 128)
                out_ref[sub * 8 + part, slot, 0] = left_ref[slot, sub, 0, :, columns]
                out_ref[sub * 8 + part, slot, 1] = right_ref[slot, sub, 0, :, columns]


def pick_roots(in_ref, table_ref, out_ref):
    for block in range(32):
        out_ref[block] = in_ref[table_ref[block]]


def join_roots(in_ref, left_ref, right_ref):
    for sub in range(4):
        for part in range(8):
            columns = slice(part * 128, part * 128 + 128)
            left_ref[sub, :, columns] = in_ref[sub * 8 + part, 0]
            right_ref[sub, :, columns] = in_ref[sub * 8 + part, 1]


def add_pair(grads_ref, theirs_ref, where_ref, own_ref, one_ref, two_ref, three_ref, four_ref):
    z, core = where_ref[0], where_ref[1]
    ahead = 1 - 2 * core

    def pair(k, parity):
        strip = lax.rem(z + 8 + k * ahead, 8) * 2 + parity
        rows = pl.ds(pl.multiple_of(strip * 16, 16), 16)
        return (grads_ref[0, rows, :].astype(F32) + theirs_ref[0, rows, :].astype(F32)).astype(BF)

    four_ref[...] = pair(4, core)
    for k, ref in ((3, three_ref), (2, two_ref), (1, one_ref)):
        for parity in range(2):
            ref[parity] = pair(k, parity)
    own_ref[...] = pair(0, core)


def add_half(both_ref, half_ref, where_ref, out_ref):
    core = where_ref[1]
    out_ref[1 - core] = both_ref[1 - core]
    out_ref[core] = (both_ref[core].astype(F32) + half_ref[...].astype(F32)).astype(BF)


def add_both(left_ref, right_ref, out_ref):
    out_ref[...] = (left_ref[...].astype(F32) + right_ref[...].astype(F32)).astype(BF)


def add_replicas(own_ref, mine_ref, theirs_ref, where_ref, out_ref):
    for column in range(4):
        columns = slice(column * 1024, column * 1024 + 1024)
        total = (
            own_ref[:, columns].astype(F32)
            + mine_ref[where_ref[1], :, columns].astype(F32)
            + theirs_ref[:, columns].astype(F32)
        ).astype(BF)
        for z in range(8):
            out_ref[z * 4 + column] = total


def place(whole, rows, z, parity):
    for sub in range(4):
        base = sub * 256 + z * 32 + parity * 16
        whole[pl.ds(pl.multiple_of(base, 16), 16), :] = rows[sub]


def products(mine_ref, other_ref, left_ref, where_ref, gram_ref, mixed_ref, whole, both):
    core = where_ref[1]
    strip = where_ref[0] * 2 + core
    for z in range(8):
        place(whole, mine_ref.at[z], z, core)
        place(whole, other_ref.at[z], z, 1 - core)
    row = lax.broadcasted_iota(jnp.int32, (64, 1024), 0)
    column = lax.broadcasted_iota(jnp.int32, (64, 1024), 1)
    chosen = (row // 16) * 256 + strip * 16 + row % 16
    both[0:64] = mine_ref[where_ref[0]].reshape(64, 1024)
    both[64:128] = jnp.where(column == chosen, 1.0, 0.0).astype(BF)
    first = lax.dot_general(
        both[...], whole[...], (((1,), (1,)), ((), ())), preferred_element_type=F32
    )
    both[0:64] = first[64:128].astype(BF)
    both[64:128] = left_ref[...].reshape(64, 1024)
    second = jnp.dot(both[...], whole[...], preferred_element_type=F32)
    left_gram = (first[0:64] * (1.0 / 1024)).astype(BF)
    right_gram = (second[0:64] * (1.0 / 1024)).astype(BF)
    for sub in range(4):
        for part in range(8):
            columns = slice(part * 128, part * 128 + 128)
            gram_ref[sub * 8 + part, 0] = left_gram[sub * 16 : sub * 16 + 16, columns]
            gram_ref[sub * 8 + part, 1] = right_gram[sub * 16 : sub * 16 + 16, columns]
    mixed_ref[...] = second[64:128].astype(BF)


def to_slots(in_ref, holder_ref, out_ref):
    for slot in range(64):
        block = holder_ref[slot]
        piece = in_ref[jnp.maximum(block, 0)]
        out_ref[slot // 2, slot % 2] = jnp.where(block >= 0, piece, jnp.zeros_like(piece))


def finish_grams(in_ref, left_ref, right_ref, left_out, right_out):
    for slot in range(2):
        for sub in range(4):
            for part in range(8):
                columns = slice(part * 128, part * 128 + 128)
                piece = sub * 8 + part
                left_out[slot, sub, 0, :, columns] = left_ref[slot, sub, 0, :, columns] + in_ref[
                    piece, slot, 0
                ].astype(F32)
                right_out[slot, sub, 0, :, columns] = right_ref[slot, sub, 0, :, columns] + in_ref[
                    piece, slot, 1
                ].astype(F32)


def pair_up(mine_ref, other_ref, where_ref, out_ref):
    out_ref[where_ref[1]] = mine_ref[...]
    out_ref[1 - where_ref[1]] = other_ref[...]


def take_parity(in_ref, where_ref, out_ref):
    out_ref[...] = in_ref[where_ref[1]]


def stack_rows(first_ref, second_ref, third_ref, last_ref, out_ref):
    for hop, ref in enumerate((first_ref, second_ref, third_ref)):
        out_ref[2 * hop] = ref[0]
        out_ref[2 * hop + 1] = ref[1]
    out_ref[6] = last_ref[...]


def right_product(pair_ref, mine_ref, other_ref, mixed_ref, where_ref, *refs):
    whole, rows = refs[4:]
    z, core = where_ref[0], where_ref[1]
    for parity in range(2):
        place(whole, pair_ref.at[parity], z, parity)
        for hop in range(3):
            ahead = (1 - 2 * core) * (hop + 1)
            place(whole, mine_ref.at[2 * hop + parity], lax.rem(z + 8 + ahead, 8), parity)
            place(whole, other_ref.at[2 * hop + parity], lax.rem(z + 8 - ahead, 8), parity)
    place(whole, mine_ref.at[6], lax.rem(z + 4, 8), core)
    place(whole, other_ref.at[6], lax.rem(z + 4, 8), 1 - core)
    product = jnp.dot(mixed_ref[...], whole[...], preferred_element_type=F32)
    rows[...] = product.astype(BF).reshape(4, 16, 1024)
    for k in range(4):
        refs[k][...] = rows[lax.rem(where_ref[2] + k, 4)]


def join_columns(*refs):
    where_ref, out_ref = refs[4:]
    for k in range(4):
        column = lax.rem(where_ref[2] + 4 - k, 4) * 1024
        out_ref[0, 0, :, pl.ds(pl.multiple_of(column, 1024), 1024)] = refs[k][...]


def exchange(value, axes):
    return lax.all_to_all(value, axes, split_axis=0, concat_axis=0, tiled=True)


def swap(value):
    return lax.ppermute(value, "c", [(0, 1), (1, 0)])


def shift(value, axis, distance):
    size = lax.axis_size(axis)
    return lax.ppermute(value, axis, [(i, (i + distance) % size) for i in range(size)])


def around(value, way):
    pairs = [(2 * z + c, 2 * ((z + way - 2 * way * c) % 8) + c) for z in range(8) for c in range(2)]
    return lax.ppermute(value, ROWS, pairs)


def step(grads, table, left_state, right_state, left_root, right_root):
    z, core = lax.axis_index("z"), lax.axis_index("c")
    where = jnp.stack([z, core, lax.axis_index("yl")]).astype(jnp.int32)
    slots = jnp.arange(64, dtype=jnp.int32)
    blocks = jnp.arange(32, dtype=jnp.int32)
    holder = jnp.sum(jnp.where(table[None, :] == slots[:, None], blocks[None, :] + 1, 0), axis=1) - 1

    theirs = swap(grads)
    both = shape((2, 16, 4096))
    own, one, two, three, four = call(
        add_pair,
        (shape((16, 4096)), both, both, both, shape((16, 4096))),
        [grads, theirs, where],
        scalars=1,
    )
    partial = around(four, 1)
    partial = call(add_half, both, [three, partial, where], scalars=1)
    partial = around(partial, 1)
    partial = call(add_both, both, [two, partial])
    partial = around(partial, 1)
    partial = call(add_both, both, [one, partial])
    partial = around(partial, 1)
    other = call(take_parity, shape((16, 4096)), [partial, 1 - where], scalars=1)
    other = swap(other)
    strip = call(
        add_replicas, shape((32, 16, 1024)), [own, partial, other, where], scalars=1
    )

    pieces = call(spread_roots, shape((32, 2, 2, 16, 128)), [left_root, right_root])
    pieces = exchange(pieces, BANDS).reshape(64, 2, 16, 128)
    picked = call(pick_roots, shape((32, 2, 16, 128)), [pieces, table], scalars=1)
    picked = exchange(picked, BANDS)
    left_rows, right_rows = call(join_roots, (shape((4, 16, 1024)), shape((4, 16, 1024))), [picked])

    mine = exchange(strip, ("z", "yl")).reshape(8, 4, 16, 1024)
    other = swap(mine)
    gram, mixed = call(
        products,
        (shape((32, 2, 16, 128)), shape((64, 1024))),
        [mine, other, left_rows, where],
        scalars=1,
        scratch=[pltpu.VMEM((1024, 1024), BF), pltpu.VMEM((128, 1024), BF)],
        flops=2 * 256 * 1024 * 1024,
    )

    gram = exchange(gram, BANDS)
    gram = call(to_slots, shape((32, 2, 2, 16, 128)), [gram, holder], scalars=1)
    gram = exchange(gram, BANDS)
    left_new, right_new = call(
        finish_grams,
        (shape(left_state.shape, F32), shape(right_state.shape, F32)),
        [gram, left_state, right_state],
    )

    theirs = swap(right_rows)
    pair = call(
        pair_up, shape((2, 4, 16, 1024)), [right_rows, theirs, where], scalars=1
    )
    rings = [around(pair, -1)]
    rings.append(around(rings[0], -1))
    rings.append(around(rings[1], -1))
    half = call(take_parity, shape((4, 16, 1024)), [rings[2], where], scalars=1)
    rings.append(around(half, -1))
    right_mine = call(stack_rows, shape((7, 4, 16, 1024)), rings)
    right_other = swap(right_mine)
    result = call(
        right_product,
        (shape((16, 1024)),) * 4,
        [pair, right_mine, right_other, mixed, where],
        scalars=1,
        scratch=[pltpu.VMEM((1024, 1024), BF), pltpu.VMEM((4, 16, 1024), BF)],
        flops=2 * 64 * 1024 * 1024,
    )
    home = [result[0]] + [shift(result[k], "yl", k) for k in range(1, 4)]
    direction = call(join_columns, shape((1, 1, 16, 4096)), [*home, where], scalars=1)
    return direction, left_new, right_new


def solution(mesh):
    fine = Mesh(mesh.devices.reshape(8, 2, 4, 2, 4), ROWS + BANDS)
    state = P(BANDS, None, ROWS, None, None)
    return jax.shard_map(
        step,
        mesh=fine,
        in_specs=(P(ROWS, BANDS, None), P(), state, state, state, state),
        out_specs=(P(BANDS, ROWS, None, None), state, state),
        check_vma=False,
    )
```

```python
import jax
import jax.numpy as jnp
from jax import lax
from jax.experimental import pallas as pl
from jax.experimental.pallas import tpu as pltpu
from jax.sharding import Mesh, PartitionSpec as P


BF = jnp.bfloat16
F32 = jnp.float32
BANDS = ("x", "yh", "yl")
ROWS = ("z", "c")
VM = pl.BlockSpec(memory_space=pltpu.VMEM)
SM = pl.BlockSpec(memory_space=pltpu.SMEM)


def call(kernel, out, inputs, scalars=0, scratch=(), flops=1000000):
    moved = sum(a.size * a.dtype.itemsize for a in inputs)
    return pl.pallas_call(
        kernel,
        out_shape=out,
        in_specs=[VM] * (len(inputs) - scalars) + [SM] * scalars,
        out_specs=jax.tree.map(lambda _: VM, out),
        scratch_shapes=scratch,
        compiler_params=pltpu.CompilerParams(vmem_limit_bytes=32 * 1024 * 1024),
        cost_estimate=pl.CostEstimate(flops=flops, bytes_accessed=moved, transcendentals=0),
    )(*inputs)


def shape(dims, dtype=BF):
    return jax.ShapeDtypeStruct(dims, dtype)


def spread_roots(left_ref, right_ref, out_ref):
    for slot in range(2):
        for sub in range(4):
            for part in range(8):
                columns = slice(part * 128, part * 128 + 128)
                out_ref[sub * 8 + part, slot, 0] = left_ref[slot, sub, 0, :, columns]
                out_ref[sub * 8 + part, slot, 1] = right_ref[slot, sub, 0, :, columns]


def pick_roots(in_ref, table_ref, out_ref):
    for block in range(32):
        out_ref[block] = in_ref[table_ref[block]]


def join_roots(in_ref, left_ref, right_ref):
    for sub in range(4):
        for part in range(8):
            columns = slice(part * 128, part * 128 + 128)
            left_ref[sub, :, columns] = in_ref[sub * 8 + part, 0]
            right_ref[sub, :, columns] = in_ref[sub * 8 + part, 1]


def add_pair(grads_ref, theirs_ref, where_ref, own_ref, one_ref, two_ref, three_ref, four_ref):
    z, core = where_ref[0], where_ref[1]
    ahead = 1 - 2 * core

    def pair(k, parity):
        strip = lax.rem(z + 8 + k * ahead, 8) * 2 + parity
        rows = pl.ds(pl.multiple_of(strip * 16, 16), 16)
        return (grads_ref[0, rows, :].astype(F32) + theirs_ref[0, rows, :].astype(F32)).astype(BF)

    four_ref[...] = pair(4, core)
    for k, ref in ((3, three_ref), (2, two_ref), (1, one_ref)):
        for parity in range(2):
            ref[parity] = pair(k, parity)
    own_ref[...] = pair(0, core)


def add_passed(two_ref, three_ref, four_ref, where_ref, out_ref):
    core = where_ref[1]
    for parity in range(2):
        out_ref[parity] = (two_ref[parity].astype(F32) + three_ref[parity].astype(F32)).astype(BF)
    out_ref[core] = (
        two_ref[core].astype(F32) + three_ref[core].astype(F32) + four_ref[...].astype(F32)
    ).astype(BF)


def add_other(one_ref, two_ref, where_ref, out_ref):
    parity = 1 - where_ref[1]
    out_ref[...] = (one_ref[parity].astype(F32) + two_ref[parity].astype(F32)).astype(BF)


def add_replicas(own_ref, one_ref, two_ref, theirs_ref, where_ref, out_ref):
    for column in range(4):
        columns = slice(column * 1024, column * 1024 + 1024)
        total = (
            own_ref[:, columns].astype(F32)
            + one_ref[where_ref[1], :, columns].astype(F32)
            + two_ref[where_ref[1], :, columns].astype(F32)
            + theirs_ref[:, columns].astype(F32)
        ).astype(BF)
        for z in range(8):
            out_ref[z * 4 + column] = total


def place(whole, rows, z, parity):
    for sub in range(4):
        base = sub * 256 + z * 32 + parity * 16
        whole[pl.ds(pl.multiple_of(base, 16), 16), :] = rows[sub]


def products(mine_ref, other_ref, left_ref, where_ref, gram_ref, mixed_ref, whole, both):
    core = where_ref[1]
    strip = where_ref[0] * 2 + core
    for z in range(8):
        place(whole, mine_ref.at[z], z, core)
        place(whole, other_ref.at[z], z, 1 - core)
    row = lax.broadcasted_iota(jnp.int32, (64, 1024), 0)
    column = lax.broadcasted_iota(jnp.int32, (64, 1024), 1)
    chosen = (row // 16) * 256 + strip * 16 + row % 16
    both[0:64] = mine_ref[where_ref[0]].reshape(64, 1024)
    both[64:128] = jnp.where(column == chosen, 1.0, 0.0).astype(BF)
    first = lax.dot_general(
        both[...], whole[...], (((1,), (1,)), ((), ())), preferred_element_type=F32
    )
    both[0:64] = first[64:128].astype(BF)
    both[64:128] = left_ref[...].reshape(64, 1024)
    second = jnp.dot(both[...], whole[...], preferred_element_type=F32)
    left_gram = (first[0:64] * (1.0 / 1024)).astype(BF)
    right_gram = (second[0:64] * (1.0 / 1024)).astype(BF)
    for sub in range(4):
        for part in range(8):
            columns = slice(part * 128, part * 128 + 128)
            gram_ref[sub * 8 + part, 0] = left_gram[sub * 16 : sub * 16 + 16, columns]
            gram_ref[sub * 8 + part, 1] = right_gram[sub * 16 : sub * 16 + 16, columns]
    mixed_ref[...] = second[64:128].astype(BF)


def to_slots(in_ref, holder_ref, out_ref):
    for slot in range(64):
        block = holder_ref[slot]
        piece = in_ref[jnp.maximum(block, 0)]
        out_ref[slot // 2, slot % 2] = jnp.where(block >= 0, piece, jnp.zeros_like(piece))


def finish_grams(in_ref, left_ref, right_ref, left_out, right_out):
    for slot in range(2):
        for sub in range(4):
            for part in range(8):
                columns = slice(part * 128, part * 128 + 128)
                piece = sub * 8 + part
                left_out[slot, sub, 0, :, columns] = left_ref[slot, sub, 0, :, columns] + in_ref[
                    piece, slot, 0
                ].astype(F32)
                right_out[slot, sub, 0, :, columns] = right_ref[slot, sub, 0, :, columns] + in_ref[
                    piece, slot, 1
                ].astype(F32)


def pair_up(mine_ref, other_ref, where_ref, out_ref):
    out_ref[where_ref[1]] = mine_ref[...]
    out_ref[1 - where_ref[1]] = other_ref[...]


def take_parity(in_ref, where_ref, out_ref):
    out_ref[...] = in_ref[where_ref[1]]


def stack_rows(first_ref, second_ref, third_ref, last_ref, out_ref):
    for hop, ref in enumerate((first_ref, second_ref, third_ref)):
        out_ref[2 * hop] = ref[0]
        out_ref[2 * hop + 1] = ref[1]
    out_ref[6] = last_ref[...]


def right_product(pair_ref, mine_ref, other_ref, mixed_ref, where_ref, out_ref, whole):
    z, core = where_ref[0], where_ref[1]
    for parity in range(2):
        place(whole, pair_ref.at[parity], z, parity)
        for hop in range(3):
            ahead = (1 - 2 * core) * (hop + 1)
            place(whole, mine_ref.at[2 * hop + parity], lax.rem(z + 8 + ahead, 8), parity)
            place(whole, other_ref.at[2 * hop + parity], lax.rem(z + 8 - ahead, 8), parity)
    place(whole, mine_ref.at[6], lax.rem(z + 4, 8), core)
    place(whole, other_ref.at[6], lax.rem(z + 4, 8), 1 - core)
    product = jnp.dot(mixed_ref[...], whole[...], preferred_element_type=F32)
    out_ref[...] = product.astype(BF).reshape(4, 16, 1024)


def join_columns(in_ref, out_ref):
    for column in range(4):
        out_ref[0, 0, :, column * 1024 : column * 1024 + 1024] = in_ref[column]


def exchange(value, axes):
    return lax.all_to_all(value, axes, split_axis=0, concat_axis=0, tiled=True)


def swap(value):
    return lax.ppermute(value, "c", [(0, 1), (1, 0)])


def around(value, way):
    pairs = [(2 * z + c, 2 * ((z + way - 2 * way * c) % 8) + c) for z in range(8) for c in range(2)]
    return lax.ppermute(value, ROWS, pairs)


def step(grads, table, left_state, right_state, left_root, right_root):
    z, core = lax.axis_index("z"), lax.axis_index("c")
    where = jnp.stack([z, core]).astype(jnp.int32)
    slots = jnp.arange(64, dtype=jnp.int32)
    blocks = jnp.arange(32, dtype=jnp.int32)
    holder = jnp.sum(jnp.where(table[None, :] == slots[:, None], blocks[None, :] + 1, 0), axis=1) - 1

    theirs = swap(grads)
    both = shape((2, 16, 4096))
    own, one, two, three, four = call(
        add_pair,
        (shape((16, 4096)), both, both, both, shape((16, 4096))),
        [grads, theirs, where],
        scalars=1,
    )
    four = around(four, 2)
    three = around(three, 1)
    one = around(one, 1)
    two = call(add_passed, both, [two, three, four, where], scalars=1)
    two = around(two, 2)
    other = call(add_other, shape((16, 4096)), [one, two, where], scalars=1)
    other = swap(other)
    strip = call(
        add_replicas, shape((32, 16, 1024)), [own, one, two, other, where], scalars=1
    )

    pieces = call(spread_roots, shape((32, 2, 2, 16, 128)), [left_root, right_root])
    pieces = exchange(pieces, BANDS).reshape(64, 2, 16, 128)
    picked = call(pick_roots, shape((32, 2, 16, 128)), [pieces, table], scalars=1)
    picked = exchange(picked, BANDS)
    left_rows, right_rows = call(join_roots, (shape((4, 16, 1024)), shape((4, 16, 1024))), [picked])

    mine = exchange(strip, ("z", "yl")).reshape(8, 4, 16, 1024)
    other = swap(mine)
    gram, mixed = call(
        products,
        (shape((32, 2, 16, 128)), shape((64, 1024))),
        [mine, other, left_rows, where],
        scalars=1,
        scratch=[pltpu.VMEM((1024, 1024), BF), pltpu.VMEM((128, 1024), BF)],
        flops=2 * 256 * 1024 * 1024,
    )

    gram = exchange(gram, BANDS)
    gram = call(to_slots, shape((32, 2, 2, 16, 128)), [gram, holder], scalars=1)
    gram = exchange(gram, BANDS)
    left_new, right_new = call(
        finish_grams,
        (shape(left_state.shape, F32), shape(right_state.shape, F32)),
        [gram, left_state, right_state],
    )

    theirs = swap(right_rows)
    pair = call(
        pair_up, shape((2, 4, 16, 1024)), [right_rows, theirs, where], scalars=1
    )
    second = around(pair, -2)
    first = around(pair, -1)
    half = call(take_parity, shape((4, 16, 1024)), [second, where], scalars=1)
    third = around(second, -1)
    last = around(half, -2)
    right_mine = call(stack_rows, shape((7, 4, 16, 1024)), [first, second, third, last])
    right_other = swap(right_mine)
    result = call(
        right_product,
        shape((4, 16, 1024)),
        [pair, right_mine, right_other, mixed, where],
        scalars=1,
        scratch=[pltpu.VMEM((1024, 1024), BF)],
        flops=2 * 64 * 1024 * 1024,
    )
    direction = call(join_columns, shape((1, 1, 16, 4096)), [exchange(result, "yl")])
    return direction, left_new, right_new


def solution(mesh):
    fine = Mesh(mesh.devices.reshape(8, 2, 4, 2, 4), ROWS + BANDS)
    state = P(BANDS, None, ROWS, None, None)
    return jax.shard_map(
        step,
        mesh=fine,
        in_specs=(P(ROWS, BANDS, None), P(), state, state, state, state),
        out_specs=(P(BANDS, ROWS, None, None), state, state),
        check_vma=False,
    )
```

```python
import functools

import jax
import jax.numpy as jnp
from jax import lax
from jax.experimental import pallas as pl
from jax.experimental.pallas import tpu as pltpu
from jax.sharding import Mesh, PartitionSpec as P


BF = jnp.bfloat16
F32 = jnp.float32
BANDS = ("x", "yh", "yl")
ROWS = ("z", "c")
VM = pl.BlockSpec(memory_space=pltpu.VMEM)
SM = pl.BlockSpec(memory_space=pltpu.SMEM)


def call(kernel, out, inputs, scalars=0, scratch=(), flops=1000000):
    moved = sum(a.size * a.dtype.itemsize for a in inputs)
    return pl.pallas_call(
        kernel,
        out_shape=out,
        in_specs=[VM] * (len(inputs) - scalars) + [SM] * scalars,
        out_specs=jax.tree.map(lambda _: VM, out),
        scratch_shapes=scratch,
        compiler_params=pltpu.CompilerParams(vmem_limit_bytes=32 * 1024 * 1024),
        cost_estimate=pl.CostEstimate(flops=flops, bytes_accessed=moved, transcendentals=0),
    )(*inputs)


def shape(dims, dtype=BF):
    return jax.ShapeDtypeStruct(dims, dtype)


def spread_roots(left_hbm, right_hbm, out_ref, left_ref, right_ref, sems):
    copies = (
        pltpu.make_async_copy(left_hbm, left_ref, sems.at[0]),
        pltpu.make_async_copy(right_hbm, right_ref, sems.at[1]),
    )
    for copy in copies:
        copy.start()
    for root, (copy, ref) in enumerate(zip(copies, (left_ref, right_ref))):
        copy.wait()
        for slot in range(2):
            for sub in range(4):
                for part in range(8):
                    columns = slice(part * 128, part * 128 + 128)
                    out_ref[sub * 8 + part, slot, root] = ref[slot, sub, 0, :, columns]


def pick_roots(in_ref, table_ref, out_ref):
    for block in range(32):
        out_ref[block] = in_ref[table_ref[block]]


def join_roots(in_ref, left_ref, right_ref):
    for sub in range(4):
        for part in range(8):
            columns = slice(part * 128, part * 128 + 128)
            left_ref[sub, :, columns] = in_ref[sub * 8 + part, 0]
            right_ref[sub, :, columns] = in_ref[sub * 8 + part, 1]


def add_pairs(wanted, grads_ref, theirs_hbm, where_ref, *refs):
    z, core = where_ref[0], where_ref[1]
    outs, theirs_ref, sems = refs[:-2], refs[-2], refs[-1]
    copies = []
    for index, (_, _, k, parity) in enumerate(wanted):
        strip = lax.rem(z + 8 + k * (1 - 2 * core), 8) * 2 + (core if parity is None else parity)
        rows = pl.ds(pl.multiple_of(strip * 16, 16), 16)
        copy = pltpu.make_async_copy(theirs_hbm.at[0, rows, :], theirs_ref.at[index], sems.at[index])
        copy.start()
        copies.append((copy, rows))
    for index, (out, place_in, _, _) in enumerate(wanted):
        copy, rows = copies[index]
        copy.wait()
        total = grads_ref[0, rows, :].astype(F32) + theirs_ref[index].astype(F32)
        if place_in is None:
            outs[out][...] = total.astype(BF)
        else:
            outs[out][place_in] = total.astype(BF)


def pair_sums(wanted, outs, grads, theirs, where):
    return pl.pallas_call(
        functools.partial(add_pairs, wanted),
        out_shape=outs,
        in_specs=[VM, pl.BlockSpec(memory_space=pltpu.HBM), SM],
        out_specs=(VM,) * len(outs),
        scratch_shapes=[
            pltpu.VMEM((len(wanted), 16, 4096), BF),
            pltpu.SemaphoreType.DMA((len(wanted),)),
        ],
        compiler_params=pltpu.CompilerParams(vmem_limit_bytes=32 * 1024 * 1024),
        cost_estimate=pl.CostEstimate(flops=1000000, bytes_accessed=2097152, transcendentals=0),
    )(grads, theirs, where)


def add_passed(two_ref, near_ref, four_ref, where_ref, out_ref):
    core = where_ref[1]
    for parity in range(2):
        out_ref[parity] = (two_ref[parity].astype(F32) + near_ref[parity].astype(F32)).astype(BF)
    out_ref[core] = (
        two_ref[core].astype(F32) + near_ref[core].astype(F32) + four_ref[...].astype(F32)
    ).astype(BF)


def add_other(near_ref, two_ref, where_ref, out_ref):
    parity = 1 - where_ref[1]
    out_ref[...] = (near_ref[2 + parity].astype(F32) + two_ref[parity].astype(F32)).astype(BF)


def add_replicas(own_ref, near_ref, two_ref, theirs_ref, where_ref, out_ref):
    for column in range(4):
        columns = slice(column * 1024, column * 1024 + 1024)
        total = (
            own_ref[:, columns].astype(F32)
            + near_ref[2 + where_ref[1], :, columns].astype(F32)
            + two_ref[where_ref[1], :, columns].astype(F32)
            + theirs_ref[:, columns].astype(F32)
        ).astype(BF)
        for z in range(8):
            out_ref[z * 4 + column] = total


def place(whole, rows, z, parity):
    for sub in range(4):
        base = sub * 256 + z * 32 + parity * 16
        whole[pl.ds(pl.multiple_of(base, 16), 16), :] = rows[sub]


def products(mine_ref, other_ref, left_ref, where_ref, gram_ref, mixed_ref, whole, both):
    core = where_ref[1]
    strip = where_ref[0] * 2 + core
    for z in range(8):
        place(whole, mine_ref.at[z], z, core)
        place(whole, other_ref.at[z], z, 1 - core)
    row = lax.broadcasted_iota(jnp.int32, (64, 1024), 0)
    column = lax.broadcasted_iota(jnp.int32, (64, 1024), 1)
    chosen = (row // 16) * 256 + strip * 16 + row % 16
    both[0:64] = mine_ref[where_ref[0]].reshape(64, 1024)
    both[64:128] = jnp.where(column == chosen, 1.0, 0.0).astype(BF)
    first = lax.dot_general(
        both[...], whole[...], (((1,), (1,)), ((), ())), preferred_element_type=F32
    )
    both[0:64] = first[64:128].astype(BF)
    both[64:128] = left_ref[...].reshape(64, 1024)
    second = jnp.dot(both[...], whole[...], preferred_element_type=F32)
    left_gram = (first[0:64] * (1.0 / 1024)).astype(BF)
    right_gram = (second[0:64] * (1.0 / 1024)).astype(BF)
    for sub in range(4):
        for part in range(8):
            columns = slice(part * 128, part * 128 + 128)
            gram_ref[sub * 8 + part, 0] = left_gram[sub * 16 : sub * 16 + 16, columns]
            gram_ref[sub * 8 + part, 1] = right_gram[sub * 16 : sub * 16 + 16, columns]
    mixed_ref[...] = second[64:128].astype(BF)


def to_slots(in_ref, holder_ref, out_ref):
    for slot in range(64):
        block = holder_ref[slot]
        piece = in_ref[jnp.maximum(block, 0)]
        out_ref[slot // 2, slot % 2] = jnp.where(block >= 0, piece, jnp.zeros_like(piece))


def finish_grams(in_ref, left_ref, right_ref, left_out, right_out):
    for slot in range(2):
        for sub in range(4):
            for part in range(8):
                columns = slice(part * 128, part * 128 + 128)
                piece = sub * 8 + part
                left_out[slot, sub, 0, :, columns] = left_ref[slot, sub, 0, :, columns] + in_ref[
                    piece, slot, 0
                ].astype(F32)
                right_out[slot, sub, 0, :, columns] = right_ref[slot, sub, 0, :, columns] + in_ref[
                    piece, slot, 1
                ].astype(F32)


def pair_up(mine_ref, other_ref, where_ref, out_ref):
    out_ref[where_ref[1]] = mine_ref[...]
    out_ref[1 - where_ref[1]] = other_ref[...]


def take_parity(in_ref, where_ref, out_ref):
    out_ref[...] = in_ref[where_ref[1]]


def stack_rows(first_ref, second_ref, third_ref, last_ref, out_ref):
    for hop, ref in enumerate((first_ref, second_ref, third_ref)):
        out_ref[2 * hop] = ref[0]
        out_ref[2 * hop + 1] = ref[1]
    out_ref[6] = last_ref[...]


def right_product(pair_ref, mine_ref, other_ref, mixed_ref, where_ref, *refs):
    whole, rows = refs[4:]
    z, core = where_ref[0], where_ref[1]
    for parity in range(2):
        place(whole, pair_ref.at[parity], z, parity)
        for hop in range(3):
            ahead = (1 - 2 * core) * (hop + 1)
            place(whole, mine_ref.at[2 * hop + parity], lax.rem(z + 8 + ahead, 8), parity)
            place(whole, other_ref.at[2 * hop + parity], lax.rem(z + 8 - ahead, 8), parity)
    place(whole, mine_ref.at[6], lax.rem(z + 4, 8), core)
    place(whole, other_ref.at[6], lax.rem(z + 4, 8), 1 - core)
    product = jnp.dot(mixed_ref[...], whole[...], preferred_element_type=F32)
    rows[...] = product.astype(BF).reshape(4, 16, 1024)
    for k in range(4):
        refs[k][...] = rows[lax.rem(where_ref[2] + k, 4)]


def join_columns(*refs):
    where_ref, out_ref = refs[4:]
    for k in range(4):
        column = lax.rem(where_ref[2] + 4 - k, 4) * 1024
        out_ref[0, 0, :, pl.ds(pl.multiple_of(column, 1024), 1024)] = refs[k][...]


def exchange(value, axes):
    return lax.all_to_all(value, axes, split_axis=0, concat_axis=0, tiled=True)


def swap(value):
    return lax.ppermute(value, "c", [(0, 1), (1, 0)])


def shift(value, axis, distance):
    size = lax.axis_size(axis)
    return lax.ppermute(value, axis, [(i, (i + distance) % size) for i in range(size)])


def around(value, way):
    pairs = [(2 * z + c, 2 * ((z + way - 2 * way * c) % 8) + c) for z in range(8) for c in range(2)]
    return lax.ppermute(value, ROWS, pairs)


def step(grads, table, left_state, right_state, left_root, right_root):
    z, core = lax.axis_index("z"), lax.axis_index("c")
    where = jnp.stack([z, core, lax.axis_index("yl")]).astype(jnp.int32)
    slots = jnp.arange(64, dtype=jnp.int32)
    blocks = jnp.arange(32, dtype=jnp.int32)
    holder = jnp.sum(jnp.where(table[None, :] == slots[:, None], blocks[None, :] + 1, 0), axis=1) - 1

    theirs = swap(grads)
    strip_shape, both = shape((16, 4096)), shape((2, 16, 4096))
    four, near = pair_sums(
        ((0, None, 4, None), (1, 0, 3, 0), (1, 1, 3, 1), (1, 2, 1, 0), (1, 3, 1, 1)),
        (strip_shape, shape((4, 16, 4096))),
        grads,
        theirs,
        where,
    )
    four = around(four, 2)
    near = around(near, 1)
    two, own = pair_sums(
        ((0, 0, 2, 0), (0, 1, 2, 1), (1, None, 0, None)),
        (both, strip_shape),
        grads,
        theirs,
        where,
    )
    two = call(add_passed, both, [two, near, four, where], scalars=1)
    two = around(two, 2)
    other = call(add_other, strip_shape, [near, two, where], scalars=1)
    other = swap(other)
    strip = call(
        add_replicas, shape((32, 16, 1024)), [own, near, two, other, where], scalars=1
    )

    pieces = pl.pallas_call(
        spread_roots,
        out_shape=shape((32, 2, 2, 16, 128)),
        in_specs=[pl.BlockSpec(memory_space=pltpu.HBM)] * 2,
        out_specs=VM,
        scratch_shapes=[
            pltpu.VMEM(left_root.shape, BF),
            pltpu.VMEM(left_root.shape, BF),
            pltpu.SemaphoreType.DMA((2,)),
        ],
        cost_estimate=pl.CostEstimate(flops=1000000, bytes_accessed=524288, transcendentals=0),
    )(left_root, right_root)
    pieces = exchange(pieces, BANDS).reshape(64, 2, 16, 128)
    picked = call(pick_roots, shape((32, 2, 16, 128)), [pieces, table], scalars=1)
    picked = exchange(picked, BANDS)
    left_rows, right_rows = call(join_roots, (shape((4, 16, 1024)), shape((4, 16, 1024))), [picked])

    mine = exchange(strip, ("z", "yl")).reshape(8, 4, 16, 1024)
    other = swap(mine)
    gram, mixed = call(
        products,
        (shape((32, 2, 16, 128)), shape((64, 1024))),
        [mine, other, left_rows, where],
        scalars=1,
        scratch=[pltpu.VMEM((1024, 1024), BF), pltpu.VMEM((128, 1024), BF)],
        flops=2 * 256 * 1024 * 1024,
    )

    gram = exchange(gram, BANDS)
    gram = call(to_slots, shape((32, 2, 2, 16, 128)), [gram, holder], scalars=1)
    gram = exchange(gram, BANDS)
    left_new, right_new = call(
        finish_grams,
        (shape(left_state.shape, F32), shape(right_state.shape, F32)),
        [gram, left_state, right_state],
    )

    theirs = swap(right_rows)
    pair = call(
        pair_up, shape((2, 4, 16, 1024)), [right_rows, theirs, where], scalars=1
    )
    second = around(pair, -2)
    first = around(pair, -1)
    half = call(take_parity, shape((4, 16, 1024)), [second, where], scalars=1)
    third = around(second, -1)
    last = around(half, -2)
    right_mine = call(stack_rows, shape((7, 4, 16, 1024)), [first, second, third, last])
    right_other = swap(right_mine)
    result = call(
        right_product,
        (shape((16, 1024)),) * 4,
        [pair, right_mine, right_other, mixed, where],
        scalars=1,
        scratch=[pltpu.VMEM((1024, 1024), BF), pltpu.VMEM((4, 16, 1024), BF)],
        flops=2 * 64 * 1024 * 1024,
    )
    home = [result[0]] + [shift(result[k], "yl", k) for k in range(1, 4)]
    direction = call(join_columns, shape((1, 1, 16, 4096)), [*home, where], scalars=1)
    return direction, left_new, right_new


def solution(mesh):
    fine = Mesh(mesh.devices.reshape(8, 2, 4, 2, 4), ROWS + BANDS)
    state = P(BANDS, None, ROWS, None, None)
    return jax.shard_map(
        step,
        mesh=fine,
        in_specs=(P(ROWS, BANDS, None), P(), state, state, state, state),
        out_specs=(P(BANDS, ROWS, None, None), state, state),
        check_vma=False,
    )
```

```python
import functools

import jax
import jax.numpy as jnp
from jax import lax
from jax.experimental import pallas as pl
from jax.experimental.pallas import tpu as pltpu
from jax.sharding import Mesh, PartitionSpec as P


BF = jnp.bfloat16
F32 = jnp.float32
BANDS = ("x", "yh", "yl")
ROWS = ("z", "c")
VM = pl.BlockSpec(memory_space=pltpu.VMEM)
SM = pl.BlockSpec(memory_space=pltpu.SMEM)


def call(kernel, out, inputs, scalars=0, scratch=(), flops=1000000):
    moved = sum(a.size * a.dtype.itemsize for a in inputs)
    return pl.pallas_call(
        kernel,
        out_shape=out,
        in_specs=[VM] * (len(inputs) - scalars) + [SM] * scalars,
        out_specs=jax.tree.map(lambda _: VM, out),
        scratch_shapes=scratch,
        compiler_params=pltpu.CompilerParams(vmem_limit_bytes=16 * 1024 * 1024),
        cost_estimate=pl.CostEstimate(flops=flops, bytes_accessed=moved, transcendentals=0),
    )(*inputs)


def shape(dims, dtype=BF):
    return jax.ShapeDtypeStruct(dims, dtype)


def spread_roots(left_hbm, right_hbm, out_ref, left_ref, right_ref, sems):
    copies = (
        pltpu.make_async_copy(left_hbm, left_ref, sems.at[0]),
        pltpu.make_async_copy(right_hbm, right_ref, sems.at[1]),
    )
    for copy in copies:
        copy.start()
    for root, (copy, ref) in enumerate(zip(copies, (left_ref, right_ref))):
        copy.wait()
        for slot in range(2):
            for sub in range(4):
                for part in range(8):
                    columns = slice(part * 128, part * 128 + 128)
                    out_ref[sub * 8 + part, slot, root] = ref[slot, sub, 0, :, columns]


def pick_roots(in_ref, table_ref, out_ref):
    for block in range(32):
        out_ref[block] = in_ref[table_ref[block]]


def join_roots(in_ref, left_ref, right_ref):
    for sub in range(4):
        for part in range(8):
            columns = slice(part * 128, part * 128 + 128)
            left_ref[sub, :, columns] = in_ref[sub * 8 + part, 0]
            right_ref[sub, :, columns] = in_ref[sub * 8 + part, 1]


def add_pairs(wanted, grads_ref, theirs_hbm, where_ref, *refs):
    z, core = where_ref[0], where_ref[1]
    outs, theirs_ref, sems = refs[:-2], refs[-2], refs[-1]
    copies = []
    for index, (_, _, k, parity) in enumerate(wanted):
        strip = lax.rem(z + 8 + k * (1 - 2 * core), 8) * 2 + (core if parity is None else parity)
        rows = pl.ds(pl.multiple_of(strip * 16, 16), 16)
        copy = pltpu.make_async_copy(theirs_hbm.at[0, rows, :], theirs_ref.at[index], sems.at[index])
        copy.start()
        copies.append((copy, rows))
    for index, (out, place_in, _, _) in enumerate(wanted):
        copy, rows = copies[index]
        copy.wait()
        total = grads_ref[0, rows, :].astype(F32) + theirs_ref[index].astype(F32)
        if place_in is None:
            outs[out][...] = total.astype(BF)
        else:
            outs[out][place_in] = total.astype(BF)


def pair_sums(wanted, outs, grads, theirs, where):
    return pl.pallas_call(
        functools.partial(add_pairs, wanted),
        out_shape=outs,
        in_specs=[VM, pl.BlockSpec(memory_space=pltpu.HBM), SM],
        out_specs=(VM,) * len(outs),
        scratch_shapes=[
            pltpu.VMEM((len(wanted), 16, 4096), BF),
            pltpu.SemaphoreType.DMA((len(wanted),)),
        ],
        compiler_params=pltpu.CompilerParams(vmem_limit_bytes=16 * 1024 * 1024),
        cost_estimate=pl.CostEstimate(flops=1000000, bytes_accessed=2097152, transcendentals=0),
    )(grads, theirs, where)


def add_passed(two_ref, near_ref, four_ref, where_ref, out_ref):
    core = where_ref[1]
    for parity in range(2):
        out_ref[parity] = (two_ref[parity].astype(F32) + near_ref[parity].astype(F32)).astype(BF)
    out_ref[core] = (
        two_ref[core].astype(F32) + near_ref[core].astype(F32) + four_ref[...].astype(F32)
    ).astype(BF)


def add_other(near_ref, two_ref, where_ref, out_ref):
    parity = 1 - where_ref[1]
    out_ref[...] = (near_ref[2 + parity].astype(F32) + two_ref[parity].astype(F32)).astype(BF)


def add_replicas(own_ref, near_ref, two_ref, theirs_ref, where_ref, out_hbm, strip, sems):
    copies = []
    for column in range(4):
        columns = slice(column * 1024, column * 1024 + 1024)
        strip[column] = (
            own_ref[:, columns].astype(F32)
            + near_ref[2 + where_ref[1], :, columns].astype(F32)
            + two_ref[where_ref[1], :, columns].astype(F32)
            + theirs_ref[:, columns].astype(F32)
        ).astype(BF)
        for z in range(8):
            copy = pltpu.make_async_copy(
                strip.at[column], out_hbm.at[z * 4 + column], sems.at[z * 4 + column]
            )
            copy.start()
            copies.append(copy)
    for copy in copies:
        copy.wait()


def place(whole, rows, z, parity):
    for sub in range(4):
        base = sub * 256 + z * 32 + parity * 16
        whole[pl.ds(pl.multiple_of(base, 16), 16), :] = rows[sub]


def products(mine_ref, other_ref, left_ref, where_ref, gram_ref, mixed_ref, whole, both):
    core = where_ref[1]
    strip = where_ref[0] * 2 + core
    for z in range(8):
        place(whole, mine_ref.at[z], z, core)
        place(whole, other_ref.at[z], z, 1 - core)
    row = lax.broadcasted_iota(jnp.int32, (64, 1024), 0)
    column = lax.broadcasted_iota(jnp.int32, (64, 1024), 1)
    chosen = (row // 16) * 256 + strip * 16 + row % 16
    both[0:64] = mine_ref[where_ref[0]].reshape(64, 1024)
    both[64:128] = jnp.where(column == chosen, 1.0, 0.0).astype(BF)
    first = lax.dot_general(
        both[...], whole[...], (((1,), (1,)), ((), ())), preferred_element_type=F32
    )
    both[0:64] = first[64:128].astype(BF)
    both[64:128] = left_ref[...].reshape(64, 1024)
    second = jnp.dot(both[...], whole[...], preferred_element_type=F32)
    left_gram = (first[0:64] * (1.0 / 1024)).astype(BF)
    right_gram = (second[0:64] * (1.0 / 1024)).astype(BF)
    for sub in range(4):
        for part in range(8):
            columns = slice(part * 128, part * 128 + 128)
            gram_ref[sub * 8 + part, 0] = left_gram[sub * 16 : sub * 16 + 16, columns]
            gram_ref[sub * 8 + part, 1] = right_gram[sub * 16 : sub * 16 + 16, columns]
    mixed_ref[...] = second[64:128].astype(BF)


def to_slots(in_ref, holder_ref, out_ref):
    for slot in range(64):
        block = holder_ref[slot]
        piece = in_ref[jnp.maximum(block, 0)]
        out_ref[slot // 2, slot % 2] = jnp.where(block >= 0, piece, jnp.zeros_like(piece))


def finish_grams(in_ref, left_ref, right_ref, left_out, right_out):
    for slot in range(2):
        for sub in range(4):
            for part in range(8):
                columns = slice(part * 128, part * 128 + 128)
                piece = sub * 8 + part
                left_out[slot, sub, 0, :, columns] = left_ref[slot, sub, 0, :, columns] + in_ref[
                    piece, slot, 0
                ].astype(F32)
                right_out[slot, sub, 0, :, columns] = right_ref[slot, sub, 0, :, columns] + in_ref[
                    piece, slot, 1
                ].astype(F32)


def pair_up(mine_ref, other_ref, where_ref, out_ref):
    out_ref[where_ref[1]] = mine_ref[...]
    out_ref[1 - where_ref[1]] = other_ref[...]


def take_parity(in_ref, where_ref, out_ref):
    out_ref[...] = in_ref[where_ref[1]]


def stack_rows(first_ref, second_ref, third_ref, last_ref, out_ref):
    for hop, ref in enumerate((first_ref, second_ref, third_ref)):
        out_ref[2 * hop] = ref[0]
        out_ref[2 * hop + 1] = ref[1]
    out_ref[6] = last_ref[...]


def right_product(pair_ref, mine_ref, other_ref, mixed_ref, where_ref, *refs):
    whole, rows = refs[4:]
    z, core = where_ref[0], where_ref[1]
    for parity in range(2):
        place(whole, pair_ref.at[parity], z, parity)
        for hop in range(3):
            ahead = (1 - 2 * core) * (hop + 1)
            place(whole, mine_ref.at[2 * hop + parity], lax.rem(z + 8 + ahead, 8), parity)
            place(whole, other_ref.at[2 * hop + parity], lax.rem(z + 8 - ahead, 8), parity)
    place(whole, mine_ref.at[6], lax.rem(z + 4, 8), core)
    place(whole, other_ref.at[6], lax.rem(z + 4, 8), 1 - core)
    product = jnp.dot(mixed_ref[...], whole[...], preferred_element_type=F32)
    rows[...] = product.astype(BF).reshape(4, 16, 1024)
    for k in range(4):
        refs[k][...] = rows[lax.rem(where_ref[2] + k, 4)]


def join_columns(*refs):
    where_ref, out_ref = refs[4:]
    for k in range(4):
        column = lax.rem(where_ref[2] + 4 - k, 4) * 1024
        out_ref[0, 0, :, pl.ds(pl.multiple_of(column, 1024), 1024)] = refs[k][...]


def exchange(value, axes):
    return lax.all_to_all(value, axes, split_axis=0, concat_axis=0, tiled=True)


def swap(value):
    return lax.ppermute(value, "c", [(0, 1), (1, 0)])


def shift(value, axis, distance):
    size = lax.axis_size(axis)
    return lax.ppermute(value, axis, [(i, (i + distance) % size) for i in range(size)])


def around(value, way):
    pairs = [(2 * z + c, 2 * ((z + way - 2 * way * c) % 8) + c) for z in range(8) for c in range(2)]
    return lax.ppermute(value, ROWS, pairs)


def step(grads, table, left_state, right_state, left_root, right_root):
    z, core = lax.axis_index("z"), lax.axis_index("c")
    where = jnp.stack([z, core, lax.axis_index("yl")]).astype(jnp.int32)
    slots = jnp.arange(64, dtype=jnp.int32)
    blocks = jnp.arange(32, dtype=jnp.int32)
    holder = jnp.sum(jnp.where(table[None, :] == slots[:, None], blocks[None, :] + 1, 0), axis=1) - 1

    theirs = swap(grads)
    strip_shape, both = shape((16, 4096)), shape((2, 16, 4096))
    four, near = pair_sums(
        ((0, None, 4, None), (1, 0, 3, 0), (1, 1, 3, 1), (1, 2, 1, 0), (1, 3, 1, 1)),
        (strip_shape, shape((4, 16, 4096))),
        grads,
        theirs,
        where,
    )
    four = around(four, 2)
    near = around(near, 1)
    two, own = pair_sums(
        ((0, 0, 2, 0), (0, 1, 2, 1), (1, None, 0, None)),
        (both, strip_shape),
        grads,
        theirs,
        where,
    )
    two = call(add_passed, both, [two, near, four, where], scalars=1)
    two = around(two, 2)
    other = call(add_other, strip_shape, [near, two, where], scalars=1)
    other = swap(other)
    strip = pl.pallas_call(
        add_replicas,
        out_shape=shape((32, 16, 1024)),
        in_specs=[VM] * 4 + [SM],
        out_specs=pl.BlockSpec(memory_space=pltpu.HBM),
        scratch_shapes=[pltpu.VMEM((4, 16, 1024), BF), pltpu.SemaphoreType.DMA((32,))],
        compiler_params=pltpu.CompilerParams(vmem_limit_bytes=16 * 1024 * 1024),
        cost_estimate=pl.CostEstimate(flops=1000000, bytes_accessed=1048576, transcendentals=0),
    )(own, near, two, other, where)

    pieces = pl.pallas_call(
        spread_roots,
        out_shape=shape((32, 2, 2, 16, 128)),
        in_specs=[pl.BlockSpec(memory_space=pltpu.HBM)] * 2,
        out_specs=VM,
        scratch_shapes=[
            pltpu.VMEM(left_root.shape, BF),
            pltpu.VMEM(left_root.shape, BF),
            pltpu.SemaphoreType.DMA((2,)),
        ],
        compiler_params=pltpu.CompilerParams(vmem_limit_bytes=16 * 1024 * 1024),
        cost_estimate=pl.CostEstimate(flops=1000000, bytes_accessed=524288, transcendentals=0),
    )(left_root, right_root)
    pieces = exchange(pieces, BANDS).reshape(64, 2, 16, 128)
    picked = call(pick_roots, shape((32, 2, 16, 128)), [pieces, table], scalars=1)
    picked = exchange(picked, BANDS)
    left_rows, right_rows = call(join_roots, (shape((4, 16, 1024)), shape((4, 16, 1024))), [picked])

    mine = exchange(strip, ("z", "yl")).reshape(8, 4, 16, 1024)
    other = swap(mine)
    gram, mixed = call(
        products,
        (shape((32, 2, 16, 128)), shape((64, 1024))),
        [mine, other, left_rows, where],
        scalars=1,
        scratch=[pltpu.VMEM((1024, 1024), BF), pltpu.VMEM((128, 1024), BF)],
        flops=2 * 256 * 1024 * 1024,
    )

    gram = exchange(gram, BANDS)
    gram = call(to_slots, shape((32, 2, 2, 16, 128)), [gram, holder], scalars=1)
    gram = exchange(gram, BANDS)
    left_new, right_new = call(
        finish_grams,
        (shape(left_state.shape, F32), shape(right_state.shape, F32)),
        [gram, left_state, right_state],
    )

    theirs = swap(right_rows)
    pair = call(
        pair_up, shape((2, 4, 16, 1024)), [right_rows, theirs, where], scalars=1
    )
    second = around(pair, -2)
    first = around(pair, -1)
    half = call(take_parity, shape((4, 16, 1024)), [second, where], scalars=1)
    third = around(second, -1)
    last = around(half, -2)
    right_mine = call(stack_rows, shape((7, 4, 16, 1024)), [first, second, third, last])
    right_other = swap(right_mine)
    result = call(
        right_product,
        (shape((16, 1024)),) * 4,
        [pair, right_mine, right_other, mixed, where],
        scalars=1,
        scratch=[pltpu.VMEM((1024, 1024), BF), pltpu.VMEM((4, 16, 1024), BF)],
        flops=2 * 64 * 1024 * 1024,
    )
    home = [result[0]] + [shift(result[k], "yl", k) for k in range(1, 4)]
    direction = call(join_columns, shape((1, 1, 16, 4096)), [*home, where], scalars=1)
    return direction, left_new, right_new


def solution(mesh):
    fine = Mesh(mesh.devices.reshape(8, 2, 4, 2, 4), ROWS + BANDS)
    state = P(BANDS, None, ROWS, None, None)
    return jax.shard_map(
        step,
        mesh=fine,
        in_specs=(P(ROWS, BANDS, None), P(), state, state, state, state),
        out_specs=(P(BANDS, ROWS, None, None), state, state),
        check_vma=False,
    )
```

```python
import functools

import jax
import jax.numpy as jnp
from jax import lax
from jax.experimental import pallas as pl
from jax.experimental.pallas import tpu as pltpu
from jax.sharding import Mesh, PartitionSpec as P


BF = jnp.bfloat16
F32 = jnp.float32
BANDS = ("x", "yh", "yl")
ROWS = ("z", "c")
VM = pl.BlockSpec(memory_space=pltpu.VMEM)
SM = pl.BlockSpec(memory_space=pltpu.SMEM)


def call(kernel, out, inputs, scalars=0, scratch=(), flops=1000000):
    moved = sum(a.size * a.dtype.itemsize for a in inputs)
    return pl.pallas_call(
        kernel,
        out_shape=out,
        in_specs=[VM] * (len(inputs) - scalars) + [SM] * scalars,
        out_specs=jax.tree.map(lambda _: VM, out),
        scratch_shapes=scratch,
        compiler_params=pltpu.CompilerParams(vmem_limit_bytes=32 * 1024 * 1024),
        cost_estimate=pl.CostEstimate(flops=flops, bytes_accessed=moved, transcendentals=0),
    )(*inputs)


def shape(dims, dtype=BF):
    return jax.ShapeDtypeStruct(dims, dtype)


def spread_roots(left_hbm, right_hbm, out_ref, left_ref, right_ref, sems):
    copies = (
        pltpu.make_async_copy(left_hbm, left_ref, sems.at[0]),
        pltpu.make_async_copy(right_hbm, right_ref, sems.at[1]),
    )
    for copy in copies:
        copy.start()
    for root, (copy, ref) in enumerate(zip(copies, (left_ref, right_ref))):
        copy.wait()
        for slot in range(2):
            for sub in range(4):
                for part in range(8):
                    columns = slice(part * 128, part * 128 + 128)
                    out_ref[sub * 8 + part, slot, root] = ref[slot, sub, 0, :, columns]


def pick_roots(in_ref, table_ref, out_ref):
    for block in range(32):
        out_ref[block] = in_ref[table_ref[block]]


def join_roots(in_ref, left_ref, right_ref):
    for sub in range(4):
        for part in range(8):
            columns = slice(part * 128, part * 128 + 128)
            left_ref[sub, :, columns] = in_ref[sub * 8 + part, 0]
            right_ref[sub, :, columns] = in_ref[sub * 8 + part, 1]


def add_pairs(wanted, grads_hbm, theirs_hbm, where_ref, *refs):
    z, core = where_ref[0], where_ref[1]
    outs, grads_ref, theirs_ref, sems = refs[:-3], *refs[-3:]
    copies = []
    for index, (_, _, k, parity) in enumerate(wanted):
        strip = lax.rem(z + 8 + k * (1 - 2 * core), 8) * 2 + (core if parity is None else parity)
        rows = pl.ds(pl.multiple_of(strip * 16, 16), 16)
        for source, (hbm, ref) in enumerate(((grads_hbm, grads_ref), (theirs_hbm, theirs_ref))):
            copy = pltpu.make_async_copy(
                hbm.at[0, rows, :], ref.at[index], sems.at[2 * index + source]
            )
            copy.start()
            copies.append(copy)
    for index, (out, place_in, _, _) in enumerate(wanted):
        copies[2 * index].wait()
        copies[2 * index + 1].wait()
        total = grads_ref[index].astype(F32) + theirs_ref[index].astype(F32)
        if place_in is None:
            outs[out][...] = total.astype(BF)
        else:
            outs[out][place_in] = total.astype(BF)


def pair_sums(wanted, outs, grads, theirs, where):
    return pl.pallas_call(
        functools.partial(add_pairs, wanted),
        out_shape=outs,
        in_specs=[pl.BlockSpec(memory_space=pltpu.HBM)] * 2 + [SM],
        out_specs=(VM,) * len(outs),
        scratch_shapes=[
            pltpu.VMEM((len(wanted), 16, 4096), BF),
            pltpu.VMEM((len(wanted), 16, 4096), BF),
            pltpu.SemaphoreType.DMA((2 * len(wanted),)),
        ],
        compiler_params=pltpu.CompilerParams(vmem_limit_bytes=65273856),
        cost_estimate=pl.CostEstimate(flops=1000000, bytes_accessed=2097152, transcendentals=0),
    )(grads, theirs, where)


def add_other(one_ref, two_ref, three_ref, where_ref, out_ref):
    parity = 1 - where_ref[1]
    out_ref[...] = (
        one_ref[parity].astype(F32) + two_ref[parity].astype(F32) + three_ref[parity].astype(F32)
    ).astype(BF)


def add_replicas(own_ref, one_ref, two_ref, three_ref, four_ref, theirs_ref, where_ref, out_ref):
    core = where_ref[1]
    for column in range(4):
        columns = slice(column * 1024, column * 1024 + 1024)
        total = own_ref[:, columns].astype(F32) + theirs_ref[:, columns].astype(F32)
        for ref in (one_ref, two_ref, three_ref):
            total = total + ref[core, :, columns].astype(F32)
        total = (total + four_ref[:, columns].astype(F32)).astype(BF)
        for z in range(8):
            out_ref[z * 4 + column] = total


def place(whole, rows, z, parity):
    for sub in range(4):
        base = sub * 256 + z * 32 + parity * 16
        whole[pl.ds(pl.multiple_of(base, 16), 16), :] = rows[sub]


def products(mine_ref, other_ref, left_ref, where_ref, gram_ref, mixed_ref, whole, both):
    core = where_ref[1]
    strip = where_ref[0] * 2 + core
    for z in range(8):
        place(whole, mine_ref.at[z], z, core)
        place(whole, other_ref.at[z], z, 1 - core)
    row = lax.broadcasted_iota(jnp.int32, (64, 1024), 0)
    column = lax.broadcasted_iota(jnp.int32, (64, 1024), 1)
    chosen = (row // 16) * 256 + strip * 16 + row % 16
    both[0:64] = mine_ref[where_ref[0]].reshape(64, 1024)
    both[64:128] = jnp.where(column == chosen, 1.0, 0.0).astype(BF)
    first = lax.dot_general(
        both[...], whole[...], (((1,), (1,)), ((), ())), preferred_element_type=F32
    )
    both[0:64] = first[64:128].astype(BF)
    both[64:128] = left_ref[...].reshape(64, 1024)
    second = jnp.dot(both[...], whole[...], preferred_element_type=F32)
    left_gram = (first[0:64] * (1.0 / 1024)).astype(BF)
    right_gram = (second[0:64] * (1.0 / 1024)).astype(BF)
    for sub in range(4):
        for part in range(8):
            columns = slice(part * 128, part * 128 + 128)
            gram_ref[sub * 8 + part, 0] = left_gram[sub * 16 : sub * 16 + 16, columns]
            gram_ref[sub * 8 + part, 1] = right_gram[sub * 16 : sub * 16 + 16, columns]
    mixed_ref[...] = second[64:128].astype(BF)


def to_slots(in_ref, holder_ref, out_ref):
    for slot in range(64):
        block = holder_ref[slot]
        piece = in_ref[jnp.maximum(block, 0)]
        out_ref[slot // 2, slot % 2] = jnp.where(block >= 0, piece, jnp.zeros_like(piece))


def finish_grams(in_ref, left_ref, right_ref, left_out, right_out):
    for slot in range(2):
        for sub in range(4):
            for part in range(8):
                columns = slice(part * 128, part * 128 + 128)
                piece = sub * 8 + part
                left_out[slot, sub, 0, :, columns] = left_ref[slot, sub, 0, :, columns] + in_ref[
                    piece, slot, 0
                ].astype(F32)
                right_out[slot, sub, 0, :, columns] = right_ref[slot, sub, 0, :, columns] + in_ref[
                    piece, slot, 1
                ].astype(F32)


def pair_up(mine_ref, other_ref, where_ref, out_ref):
    out_ref[where_ref[1]] = mine_ref[...]
    out_ref[1 - where_ref[1]] = other_ref[...]


def take_parity(in_ref, where_ref, out_ref):
    out_ref[...] = in_ref[where_ref[1]]


def stack_rows(first_ref, second_ref, third_ref, last_ref, out_ref):
    for hop, ref in enumerate((first_ref, second_ref, third_ref)):
        out_ref[2 * hop] = ref[0]
        out_ref[2 * hop + 1] = ref[1]
    out_ref[6] = last_ref[...]


def right_product(pair_ref, mine_ref, other_ref, mixed_ref, where_ref, *refs):
    whole, rows = refs[4:]
    z, core = where_ref[0], where_ref[1]
    for parity in range(2):
        place(whole, pair_ref.at[parity], z, parity)
        for hop in range(3):
            ahead = (1 - 2 * core) * (hop + 1)
            place(whole, mine_ref.at[2 * hop + parity], lax.rem(z + 8 + ahead, 8), parity)
            place(whole, other_ref.at[2 * hop + parity], lax.rem(z + 8 - ahead, 8), parity)
    place(whole, mine_ref.at[6], lax.rem(z + 4, 8), core)
    place(whole, other_ref.at[6], lax.rem(z + 4, 8), 1 - core)
    product = jnp.dot(mixed_ref[...], whole[...], preferred_element_type=F32)
    rows[...] = product.astype(BF).reshape(4, 16, 1024)
    for k in range(4):
        refs[k][...] = rows[lax.rem(where_ref[2] + k, 4)]


def join_columns(*refs):
    where_ref, out_ref = refs[4:]
    for k in range(4):
        column = lax.rem(where_ref[2] + 4 - k, 4) * 1024
        out_ref[0, 0, :, pl.ds(pl.multiple_of(column, 1024), 1024)] = refs[k][...]


def exchange(value, axes):
    return lax.all_to_all(value, axes, split_axis=0, concat_axis=0, tiled=True)


def swap(value):
    return lax.ppermute(value, "c", [(0, 1), (1, 0)])


def shift(value, axis, distance):
    size = lax.axis_size(axis)
    return lax.ppermute(value, axis, [(i, (i + distance) % size) for i in range(size)])


def around(value, way):
    pairs = [(2 * z + c, 2 * ((z + way - 2 * way * c) % 8) + c) for z in range(8) for c in range(2)]
    return lax.ppermute(value, ROWS, pairs)


def step(grads, table, left_state, right_state, left_root, right_root):
    z, core = lax.axis_index("z"), lax.axis_index("c")
    where = jnp.stack([z, core, lax.axis_index("yl")]).astype(jnp.int32)
    slots = jnp.arange(64, dtype=jnp.int32)
    blocks = jnp.arange(32, dtype=jnp.int32)
    holder = jnp.sum(jnp.where(table[None, :] == slots[:, None], blocks[None, :] + 1, 0), axis=1) - 1

    theirs = swap(grads)
    strip_shape, both = shape((16, 4096)), shape((2, 16, 4096))
    three, four = pair_sums(
        ((0, 0, 3, 0), (0, 1, 3, 1), (1, None, 4, None)),
        (both, strip_shape),
        grads,
        theirs,
        where,
    )
    three = around(three, 3)
    four = around(four, 4)
    two, one, own = pair_sums(
        ((0, 0, 2, 0), (0, 1, 2, 1), (1, 0, 1, 0), (1, 1, 1, 1), (2, None, 0, None)),
        (both, both, strip_shape),
        grads,
        theirs,
        where,
    )
    two = around(two, 2)
    one = around(one, 1)
    other = call(add_other, strip_shape, [one, two, three, where], scalars=1)
    other = swap(other)
    strip = call(
        add_replicas,
        shape((32, 16, 1024)),
        [own, one, two, three, four, other, where],
        scalars=1,
    )

    pieces = pl.pallas_call(
        spread_roots,
        out_shape=shape((32, 2, 2, 16, 128)),
        in_specs=[pl.BlockSpec(memory_space=pltpu.HBM)] * 2,
        out_specs=VM,
        scratch_shapes=[
            pltpu.VMEM(left_root.shape, BF),
            pltpu.VMEM(left_root.shape, BF),
            pltpu.SemaphoreType.DMA((2,)),
        ],
        cost_estimate=pl.CostEstimate(flops=1000000, bytes_accessed=524288, transcendentals=0),
    )(left_root, right_root)
    pieces = exchange(pieces, BANDS).reshape(64, 2, 16, 128)
    picked = call(pick_roots, shape((32, 2, 16, 128)), [pieces, table], scalars=1)
    picked = exchange(picked, BANDS)
    left_rows, right_rows = call(join_roots, (shape((4, 16, 1024)), shape((4, 16, 1024))), [picked])

    mine = exchange(strip, ("z", "yl")).reshape(8, 4, 16, 1024)
    other = swap(mine)
    gram, mixed = call(
        products,
        (shape((32, 2, 16, 128)), shape((64, 1024))),
        [mine, other, left_rows, where],
        scalars=1,
        scratch=[pltpu.VMEM((1024, 1024), BF), pltpu.VMEM((128, 1024), BF)],
        flops=2 * 256 * 1024 * 1024,
    )

    gram = exchange(gram, BANDS)
    gram = call(to_slots, shape((32, 2, 2, 16, 128)), [gram, holder], scalars=1)
    gram = exchange(gram, BANDS)
    left_new, right_new = call(
        finish_grams,
        (shape(left_state.shape, F32), shape(right_state.shape, F32)),
        [gram, left_state, right_state],
    )

    theirs = swap(right_rows)
    pair = call(
        pair_up, shape((2, 4, 16, 1024)), [right_rows, theirs, where], scalars=1
    )
    second = around(pair, -2)
    first = around(pair, -1)
    half = call(take_parity, shape((4, 16, 1024)), [second, where], scalars=1)
    third = around(second, -1)
    last = around(half, -2)
    right_mine = call(stack_rows, shape((7, 4, 16, 1024)), [first, second, third, last])
    right_other = swap(right_mine)
    result = call(
        right_product,
        (shape((16, 1024)),) * 4,
        [pair, right_mine, right_other, mixed, where],
        scalars=1,
        scratch=[pltpu.VMEM((1024, 1024), BF), pltpu.VMEM((4, 16, 1024), BF)],
        flops=2 * 64 * 1024 * 1024,
    )
    home = [result[0]] + [shift(result[k], "yl", k) for k in range(1, 4)]
    direction = call(join_columns, shape((1, 1, 16, 4096)), [*home, where], scalars=1)
    return direction, left_new, right_new


def solution(mesh):
    fine = Mesh(mesh.devices.reshape(8, 2, 4, 2, 4), ROWS + BANDS)
    state = P(BANDS, None, ROWS, None, None)
    return jax.shard_map(
        step,
        mesh=fine,
        in_specs=(P(ROWS, BANDS, None), P(), state, state, state, state),
        out_specs=(P(BANDS, ROWS, None, None), state, state),
        check_vma=False,
    )
```

```python
import functools

import jax
import jax.numpy as jnp
from jax import lax
from jax.experimental import pallas as pl
from jax.experimental.pallas import tpu as pltpu
from jax.sharding import Mesh, PartitionSpec as P


BF = jnp.bfloat16
F32 = jnp.float32
BANDS = ("x", "yh", "yl")
ROWS = ("z", "c")
VM = pl.BlockSpec(memory_space=pltpu.VMEM)
SM = pl.BlockSpec(memory_space=pltpu.SMEM)


def call(kernel, out, inputs, scalars=0, scratch=(), flops=1000000):
    moved = sum(a.size * a.dtype.itemsize for a in inputs)
    return pl.pallas_call(
        kernel,
        out_shape=out,
        in_specs=[VM] * (len(inputs) - scalars) + [SM] * scalars,
        out_specs=jax.tree.map(lambda _: VM, out),
        scratch_shapes=scratch,
        compiler_params=pltpu.CompilerParams(vmem_limit_bytes=32 * 1024 * 1024),
        cost_estimate=pl.CostEstimate(flops=flops, bytes_accessed=moved, transcendentals=0),
    )(*inputs)


def shape(dims, dtype=BF):
    return jax.ShapeDtypeStruct(dims, dtype)


def spread_roots(left_hbm, right_hbm, out_ref, left_ref, right_ref, sems):
    copies = (
        pltpu.make_async_copy(left_hbm, left_ref, sems.at[0]),
        pltpu.make_async_copy(right_hbm, right_ref, sems.at[1]),
    )
    for copy in copies:
        copy.start()
    for root, (copy, ref) in enumerate(zip(copies, (left_ref, right_ref))):
        copy.wait()
        for slot in range(2):
            for sub in range(4):
                for part in range(8):
                    columns = slice(part * 128, part * 128 + 128)
                    out_ref[sub * 8 + part, slot, root] = ref[slot, sub, 0, :, columns]


def pick_roots(in_ref, table_ref, out_ref):
    for block in range(32):
        out_ref[block] = in_ref[table_ref[block]]


def join_roots(in_ref, left_ref, right_ref):
    for sub in range(4):
        for part in range(8):
            columns = slice(part * 128, part * 128 + 128)
            left_ref[sub, :, columns] = in_ref[sub * 8 + part, 0]
            right_ref[sub, :, columns] = in_ref[sub * 8 + part, 1]


def add_pairs(wanted, grads_ref, theirs_hbm, where_ref, *refs):
    z, core = where_ref[0], where_ref[1]
    outs, theirs_ref, sems = refs[:-2], refs[-2], refs[-1]
    copies = []
    for index, (_, _, k, parity) in enumerate(wanted):
        strip = lax.rem(z + 8 + k * (1 - 2 * core), 8) * 2 + (core if parity is None else parity)
        rows = pl.ds(pl.multiple_of(strip * 16, 16), 16)
        copy = pltpu.make_async_copy(theirs_hbm.at[0, rows, :], theirs_ref.at[index], sems.at[index])
        copy.start()
        copies.append((copy, rows))
    for index, (out, place_in, _, _) in enumerate(wanted):
        copy, rows = copies[index]
        copy.wait()
        total = grads_ref[0, rows, :].astype(F32) + theirs_ref[index].astype(F32)
        if place_in is None:
            outs[out][...] = total.astype(BF)
        else:
            outs[out][place_in] = total.astype(BF)


def pair_sums(wanted, outs, grads, theirs, where):
    return pl.pallas_call(
        functools.partial(add_pairs, wanted),
        out_shape=outs,
        in_specs=[VM, pl.BlockSpec(memory_space=pltpu.HBM), SM],
        out_specs=(VM,) * len(outs),
        scratch_shapes=[
            pltpu.VMEM((len(wanted), 16, 4096), BF),
            pltpu.SemaphoreType.DMA((len(wanted),)),
        ],
        compiler_params=pltpu.CompilerParams(vmem_limit_bytes=32 * 1024 * 1024),
        cost_estimate=pl.CostEstimate(flops=1000000, bytes_accessed=2097152, transcendentals=0),
    )(grads, theirs, where)


def add_other(one_ref, two_ref, three_ref, where_ref, out_ref):
    parity = 1 - where_ref[1]
    out_ref[...] = (
        one_ref[parity].astype(F32) + two_ref[parity].astype(F32) + three_ref[parity].astype(F32)
    ).astype(BF)


def add_replicas(own_ref, one_ref, two_ref, three_ref, four_ref, theirs_ref, where_ref, out_ref):
    core = where_ref[1]
    for column in range(4):
        columns = slice(column * 1024, column * 1024 + 1024)
        total = own_ref[:, columns].astype(F32) + theirs_ref[:, columns].astype(F32)
        for ref in (one_ref, two_ref, three_ref):
            total = total + ref[core, :, columns].astype(F32)
        total = (total + four_ref[:, columns].astype(F32)).astype(BF)
        for z in range(8):
            out_ref[z * 4 + column] = total


def place(whole, rows, z, parity):
    for sub in range(4):
        base = sub * 256 + z * 32 + parity * 16
        whole[pl.ds(pl.multiple_of(base, 16), 16), :] = rows[sub]


def products(mine_ref, other_ref, left_ref, where_ref, gram_ref, mixed_ref, whole, both):
    core = where_ref[1]
    strip = where_ref[0] * 2 + core
    for z in range(8):
        place(whole, mine_ref.at[z], z, core)
        place(whole, other_ref.at[z], z, 1 - core)
    row = lax.broadcasted_iota(jnp.int32, (64, 1024), 0)
    column = lax.broadcasted_iota(jnp.int32, (64, 1024), 1)
    chosen = (row // 16) * 256 + strip * 16 + row % 16
    both[0:64] = mine_ref[where_ref[0]].reshape(64, 1024)
    both[64:128] = jnp.where(column == chosen, 1.0, 0.0).astype(BF)
    first = lax.dot_general(
        both[...], whole[...], (((1,), (1,)), ((), ())), preferred_element_type=F32
    )
    both[0:64] = first[64:128].astype(BF)
    both[64:128] = left_ref[...].reshape(64, 1024)
    second = jnp.dot(both[...], whole[...], preferred_element_type=F32)
    left_gram = (first[0:64] * (1.0 / 1024)).astype(BF)
    right_gram = (second[0:64] * (1.0 / 1024)).astype(BF)
    for sub in range(4):
        for part in range(8):
            columns = slice(part * 128, part * 128 + 128)
            gram_ref[sub * 8 + part, 0] = left_gram[sub * 16 : sub * 16 + 16, columns]
            gram_ref[sub * 8 + part, 1] = right_gram[sub * 16 : sub * 16 + 16, columns]
    mixed_ref[...] = second[64:128].astype(BF)


def to_slots(in_ref, holder_ref, out_ref):
    for slot in range(64):
        block = holder_ref[slot]
        piece = in_ref[jnp.maximum(block, 0)]
        out_ref[slot // 2, slot % 2] = jnp.where(block >= 0, piece, jnp.zeros_like(piece))


def finish_grams(in_ref, left_ref, right_ref, left_out, right_out):
    for slot in range(2):
        for sub in range(4):
            for part in range(8):
                columns = slice(part * 128, part * 128 + 128)
                piece = sub * 8 + part
                left_out[slot, sub, 0, :, columns] = left_ref[slot, sub, 0, :, columns] + in_ref[
                    piece, slot, 0
                ].astype(F32)
                right_out[slot, sub, 0, :, columns] = right_ref[slot, sub, 0, :, columns] + in_ref[
                    piece, slot, 1
                ].astype(F32)


def pair_up(mine_ref, other_ref, where_ref, out_ref):
    out_ref[where_ref[1]] = mine_ref[...]
    out_ref[1 - where_ref[1]] = other_ref[...]


def pick_relay(first_ref, third_ref, where_ref, out_ref):
    out_ref[0] = first_ref[0]
    out_ref[1] = first_ref[1]
    out_ref[2] = third_ref[where_ref[1]]


def stack_rows(first_ref, relayed_ref, third_ref, out_ref):
    for parity in range(2):
        out_ref[parity] = first_ref[parity]
        out_ref[2 + parity] = relayed_ref[parity]
        out_ref[4 + parity] = third_ref[parity]
    out_ref[6] = relayed_ref[2]


def right_product(pair_ref, mine_ref, other_ref, mixed_ref, where_ref, *refs):
    whole, rows = refs[4:]
    z, core = where_ref[0], where_ref[1]
    for parity in range(2):
        place(whole, pair_ref.at[parity], z, parity)
        for hop in range(3):
            ahead = (1 - 2 * core) * (hop + 1)
            place(whole, mine_ref.at[2 * hop + parity], lax.rem(z + 8 + ahead, 8), parity)
            place(whole, other_ref.at[2 * hop + parity], lax.rem(z + 8 - ahead, 8), parity)
    place(whole, mine_ref.at[6], lax.rem(z + 4, 8), core)
    place(whole, other_ref.at[6], lax.rem(z + 4, 8), 1 - core)
    product = jnp.dot(mixed_ref[...], whole[...], preferred_element_type=F32)
    rows[...] = product.astype(BF).reshape(4, 16, 1024)
    for k in range(4):
        refs[k][...] = rows[lax.rem(where_ref[2] + k, 4)]


def join_columns(*refs):
    where_ref, out_ref = refs[4:]
    for k in range(4):
        column = lax.rem(where_ref[2] + 4 - k, 4) * 1024
        out_ref[0, 0, :, pl.ds(pl.multiple_of(column, 1024), 1024)] = refs[k][...]


def exchange(value, axes):
    return lax.all_to_all(value, axes, split_axis=0, concat_axis=0, tiled=True)


def swap(value):
    return lax.ppermute(value, "c", [(0, 1), (1, 0)])


def shift(value, axis, distance):
    size = lax.axis_size(axis)
    return lax.ppermute(value, axis, [(i, (i + distance) % size) for i in range(size)])


def around(value, way):
    pairs = [(2 * z + c, 2 * ((z + way - 2 * way * c) % 8) + c) for z in range(8) for c in range(2)]
    return lax.ppermute(value, ROWS, pairs)


def step(grads, table, left_state, right_state, left_root, right_root):
    z, core = lax.axis_index("z"), lax.axis_index("c")
    where = jnp.stack([z, core, lax.axis_index("yl")]).astype(jnp.int32)
    slots = jnp.arange(64, dtype=jnp.int32)
    blocks = jnp.arange(32, dtype=jnp.int32)
    holder = jnp.sum(jnp.where(table[None, :] == slots[:, None], blocks[None, :] + 1, 0), axis=1) - 1

    theirs = swap(grads)
    strip_shape, both = shape((16, 4096)), shape((2, 16, 4096))
    three, four = pair_sums(
        ((0, 0, 3, 0), (0, 1, 3, 1), (1, None, 4, None)),
        (both, strip_shape),
        grads,
        theirs,
        where,
    )
    three = around(three, 3)
    four = around(four, 4)
    two, one, own = pair_sums(
        ((0, 0, 2, 0), (0, 1, 2, 1), (1, 0, 1, 0), (1, 1, 1, 1), (2, None, 0, None)),
        (both, both, strip_shape),
        grads,
        theirs,
        where,
    )
    two = around(two, 2)
    one = around(one, 1)
    other = call(add_other, strip_shape, [one, two, three, where], scalars=1)
    other = swap(other)
    strip = call(
        add_replicas,
        shape((32, 16, 1024)),
        [own, one, two, three, four, other, where],
        scalars=1,
    )

    pieces = pl.pallas_call(
        spread_roots,
        out_shape=shape((32, 2, 2, 16, 128)),
        in_specs=[pl.BlockSpec(memory_space=pltpu.HBM)] * 2,
        out_specs=VM,
        scratch_shapes=[
            pltpu.VMEM(left_root.shape, BF),
            pltpu.VMEM(left_root.shape, BF),
            pltpu.SemaphoreType.DMA((2,)),
        ],
        cost_estimate=pl.CostEstimate(flops=1000000, bytes_accessed=524288, transcendentals=0),
    )(left_root, right_root)
    pieces = exchange(pieces, BANDS).reshape(64, 2, 16, 128)
    picked = call(pick_roots, shape((32, 2, 16, 128)), [pieces, table], scalars=1)
    picked = exchange(picked, BANDS)
    left_rows, right_rows = call(join_roots, (shape((4, 16, 1024)), shape((4, 16, 1024))), [picked])

    mine = exchange(strip, ("z", "yl")).reshape(8, 4, 16, 1024)
    other = swap(mine)
    gram, mixed = call(
        products,
        (shape((32, 2, 16, 128)), shape((64, 1024))),
        [mine, other, left_rows, where],
        scalars=1,
        scratch=[pltpu.VMEM((1024, 1024), BF), pltpu.VMEM((128, 1024), BF)],
        flops=2 * 256 * 1024 * 1024,
    )

    gram = exchange(gram, BANDS)
    gram = call(to_slots, shape((32, 2, 2, 16, 128)), [gram, holder], scalars=1)
    gram = exchange(gram, BANDS)
    left_new, right_new = call(
        finish_grams,
        (shape(left_state.shape, F32), shape(right_state.shape, F32)),
        [gram, left_state, right_state],
    )

    theirs = swap(right_rows)
    pair = call(
        pair_up, shape((2, 4, 16, 1024)), [right_rows, theirs, where], scalars=1
    )
    third = around(pair, -3)
    first = around(pair, -1)
    relay = call(pick_relay, shape((3, 4, 16, 1024)), [first, third, where], scalars=1)
    relay = around(relay, -1)
    right_mine = call(stack_rows, shape((7, 4, 16, 1024)), [first, relay, third])
    right_other = swap(right_mine)
    result = call(
        right_product,
        (shape((16, 1024)),) * 4,
        [pair, right_mine, right_other, mixed, where],
        scalars=1,
        scratch=[pltpu.VMEM((1024, 1024), BF), pltpu.VMEM((4, 16, 1024), BF)],
        flops=2 * 64 * 1024 * 1024,
    )
    home = [result[0]] + [shift(result[k], "yl", k) for k in range(1, 4)]
    direction = call(join_columns, shape((1, 1, 16, 4096)), [*home, where], scalars=1)
    return direction, left_new, right_new


def solution(mesh):
    fine = Mesh(mesh.devices.reshape(8, 2, 4, 2, 4), ROWS + BANDS)
    state = P(BANDS, None, ROWS, None, None)
    return jax.shard_map(
        step,
        mesh=fine,
        in_specs=(P(ROWS, BANDS, None), P(), state, state, state, state),
        out_specs=(P(BANDS, ROWS, None, None), state, state),
        check_vma=False,
    )
```

```python
import functools

import jax
import jax.numpy as jnp
from jax import lax
from jax.experimental import pallas as pl
from jax.experimental.pallas import tpu as pltpu
from jax.sharding import Mesh, PartitionSpec as P


BF = jnp.bfloat16
F32 = jnp.float32
BANDS = ("x", "yh", "yl")
ROWS = ("z", "c")
VM = pl.BlockSpec(memory_space=pltpu.VMEM)
SM = pl.BlockSpec(memory_space=pltpu.SMEM)


def call(kernel, out, inputs, scalars=0, scratch=(), flops=1000000):
    moved = sum(a.size * a.dtype.itemsize for a in inputs)
    return pl.pallas_call(
        kernel,
        out_shape=out,
        in_specs=[VM] * (len(inputs) - scalars) + [SM] * scalars,
        out_specs=jax.tree.map(lambda _: VM, out),
        scratch_shapes=scratch,
        compiler_params=pltpu.CompilerParams(vmem_limit_bytes=32 * 1024 * 1024),
        cost_estimate=pl.CostEstimate(flops=flops, bytes_accessed=moved, transcendentals=0),
    )(*inputs)


def shape(dims, dtype=BF):
    return jax.ShapeDtypeStruct(dims, dtype)


def spread_roots(left_hbm, right_hbm, out_ref, left_ref, right_ref, sems):
    copies = (
        pltpu.make_async_copy(left_hbm, left_ref, sems.at[0]),
        pltpu.make_async_copy(right_hbm, right_ref, sems.at[1]),
    )
    for copy in copies:
        copy.start()
    for root, (copy, ref) in enumerate(zip(copies, (left_ref, right_ref))):
        copy.wait()
        for slot in range(2):
            for sub in range(4):
                for part in range(8):
                    columns = slice(part * 128, part * 128 + 128)
                    out_ref[sub * 8 + part, slot, root] = ref[slot, sub, 0, :, columns]


def pick_roots(in_ref, table_ref, out_ref):
    for block in range(32):
        out_ref[block] = in_ref[table_ref[block]]


def join_roots(in_ref, left_ref, right_ref):
    for sub in range(4):
        for part in range(8):
            columns = slice(part * 128, part * 128 + 128)
            left_ref[sub, :, columns] = in_ref[sub * 8 + part, 0]
            right_ref[sub, :, columns] = in_ref[sub * 8 + part, 1]


def add_pairs(wanted, grads_ref, theirs_hbm, where_ref, *refs):
    z, core = where_ref[0], where_ref[1]
    outs, theirs_ref, sems = refs[:-2], refs[-2], refs[-1]
    copies = []
    for index, (_, _, k, parity) in enumerate(wanted):
        strip = lax.rem(z + 8 + k * (1 - 2 * core), 8) * 2 + (core if parity is None else parity)
        rows = pl.ds(pl.multiple_of(strip * 16, 16), 16)
        copy = pltpu.make_async_copy(theirs_hbm.at[0, rows, :], theirs_ref.at[index], sems.at[index])
        copy.start()
        copies.append((copy, rows))
    for index, (out, place_in, _, _) in enumerate(wanted):
        copy, rows = copies[index]
        copy.wait()
        total = grads_ref[0, rows, :].astype(F32) + theirs_ref[index].astype(F32)
        if place_in is None:
            outs[out][...] = total.astype(BF)
        else:
            outs[out][place_in] = total.astype(BF)


def pair_sums(wanted, outs, grads, theirs, where):
    return pl.pallas_call(
        functools.partial(add_pairs, wanted),
        out_shape=outs,
        in_specs=[VM, pl.BlockSpec(memory_space=pltpu.HBM), SM],
        out_specs=(VM,) * len(outs),
        scratch_shapes=[
            pltpu.VMEM((len(wanted), 16, 4096), BF),
            pltpu.SemaphoreType.DMA((len(wanted),)),
        ],
        compiler_params=pltpu.CompilerParams(vmem_limit_bytes=32 * 1024 * 1024),
        cost_estimate=pl.CostEstimate(flops=1000000, bytes_accessed=2097152, transcendentals=0),
    )(grads, theirs, where)


def add_other(one_ref, two_ref, three_ref, where_ref, out_ref):
    parity = 1 - where_ref[1]
    out_ref[...] = (
        one_ref[parity].astype(F32) + two_ref[parity].astype(F32) + three_ref[parity].astype(F32)
    ).astype(BF)


def add_replicas(own_ref, one_ref, two_ref, three_ref, four_ref, theirs_ref, where_ref, out_ref):
    core = where_ref[1]
    for column in range(4):
        columns = slice(column * 1024, column * 1024 + 1024)
        total = own_ref[:, columns].astype(F32) + theirs_ref[:, columns].astype(F32)
        for ref in (one_ref, two_ref, three_ref):
            total = total + ref[core, :, columns].astype(F32)
        total = (total + four_ref[:, columns].astype(F32)).astype(BF)
        for z in range(8):
            out_ref[z * 4 + column] = total


def place(whole, rows, z, parity):
    for sub in range(4):
        base = sub * 256 + z * 32 + parity * 16
        whole[pl.ds(pl.multiple_of(base, 16), 16), :] = rows[sub]


def products(mine_ref, other_ref, left_ref, where_ref, gram_ref, mixed_ref, whole, both):
    core = where_ref[1]
    strip = where_ref[0] * 2 + core
    for z in range(8):
        place(whole, mine_ref.at[z], z, core)
        place(whole, other_ref.at[z], z, 1 - core)
    row = lax.broadcasted_iota(jnp.int32, (64, 1024), 0)
    column = lax.broadcasted_iota(jnp.int32, (64, 1024), 1)
    chosen = (row // 16) * 256 + strip * 16 + row % 16
    both[0:64] = mine_ref[where_ref[0]].reshape(64, 1024)
    both[64:128] = jnp.where(column == chosen, 1.0, 0.0).astype(BF)
    first = lax.dot_general(
        both[...], whole[...], (((1,), (1,)), ((), ())), preferred_element_type=F32
    )
    both[0:64] = first[64:128].astype(BF)
    both[64:128] = left_ref[...].reshape(64, 1024)
    second = jnp.dot(both[...], whole[...], preferred_element_type=F32)
    left_gram = (first[0:64] * (1.0 / 1024)).astype(BF)
    right_gram = (second[0:64] * (1.0 / 1024)).astype(BF)
    for sub in range(4):
        for part in range(8):
            columns = slice(part * 128, part * 128 + 128)
            gram_ref[sub * 8 + part, 0] = left_gram[sub * 16 : sub * 16 + 16, columns]
            gram_ref[sub * 8 + part, 1] = right_gram[sub * 16 : sub * 16 + 16, columns]
    mixed_ref[...] = second[64:128].astype(BF)


def to_slots(in_ref, holder_ref, out_ref):
    for slot in range(64):
        block = holder_ref[slot]
        piece = in_ref[jnp.maximum(block, 0)]
        out_ref[slot // 2, slot % 2] = jnp.where(block >= 0, piece, jnp.zeros_like(piece))


def finish_grams(in_ref, left_ref, right_ref, left_out, right_out):
    for slot in range(2):
        for sub in range(4):
            for part in range(8):
                columns = slice(part * 128, part * 128 + 128)
                piece = sub * 8 + part
                left_out[slot, sub, 0, :, columns] = left_ref[slot, sub, 0, :, columns] + in_ref[
                    piece, slot, 0
                ].astype(F32)
                right_out[slot, sub, 0, :, columns] = right_ref[slot, sub, 0, :, columns] + in_ref[
                    piece, slot, 1
                ].astype(F32)


def pair_up(mine_ref, other_ref, where_ref, out_ref):
    out_ref[where_ref[1]] = mine_ref[...]
    out_ref[1 - where_ref[1]] = other_ref[...]


def take_parity(in_ref, where_ref, out_ref):
    out_ref[...] = in_ref[where_ref[1]]


def stack_rows(first_ref, second_ref, third_ref, last_ref, out_ref):
    for hop, ref in enumerate((first_ref, second_ref, third_ref)):
        out_ref[2 * hop] = ref[0]
        out_ref[2 * hop + 1] = ref[1]
    out_ref[6] = last_ref[...]


def right_product(pair_ref, mine_ref, other_ref, mixed_ref, where_ref, *refs):
    whole, rows = refs[4:]
    z, core = where_ref[0], where_ref[1]
    for parity in range(2):
        place(whole, pair_ref.at[parity], z, parity)
        for hop in range(3):
            ahead = (1 - 2 * core) * (hop + 1)
            place(whole, mine_ref.at[2 * hop + parity], lax.rem(z + 8 + ahead, 8), parity)
            place(whole, other_ref.at[2 * hop + parity], lax.rem(z + 8 - ahead, 8), parity)
    place(whole, mine_ref.at[6], lax.rem(z + 4, 8), core)
    place(whole, other_ref.at[6], lax.rem(z + 4, 8), 1 - core)
    product = jnp.dot(mixed_ref[...], whole[...], preferred_element_type=F32)
    rows[...] = product.astype(BF).reshape(4, 16, 1024)
    for k in range(4):
        refs[k][...] = rows[lax.rem(where_ref[2] + k, 4)]


def join_columns(*refs):
    where_ref, out_ref = refs[4:]
    for k in range(4):
        column = lax.rem(where_ref[2] + 4 - k, 4) * 1024
        out_ref[0, 0, :, pl.ds(pl.multiple_of(column, 1024), 1024)] = refs[k][...]


def exchange(value, axes):
    return lax.all_to_all(value, axes, split_axis=0, concat_axis=0, tiled=True)


def swap(value):
    return lax.ppermute(value, "c", [(0, 1), (1, 0)])


def shift(value, axis, distance):
    size = lax.axis_size(axis)
    return lax.ppermute(value, axis, [(i, (i + distance) % size) for i in range(size)])


def around(value, way):
    pairs = [(2 * z + c, 2 * ((z + way - 2 * way * c) % 8) + c) for z in range(8) for c in range(2)]
    return lax.ppermute(value, ROWS, pairs)


def step(grads, table, left_state, right_state, left_root, right_root):
    z, core = lax.axis_index("z"), lax.axis_index("c")
    where = jnp.stack([z, core, lax.axis_index("yl")]).astype(jnp.int32)
    slots = jnp.arange(64, dtype=jnp.int32)
    blocks = jnp.arange(32, dtype=jnp.int32)
    holder = jnp.sum(jnp.where(table[None, :] == slots[:, None], blocks[None, :] + 1, 0), axis=1) - 1

    theirs = swap(grads)
    strip_shape, both = shape((16, 4096)), shape((2, 16, 4096))
    three, four = pair_sums(
        ((0, 0, 3, 0), (0, 1, 3, 1), (1, None, 4, None)),
        (both, strip_shape),
        grads,
        theirs,
        where,
    )
    three = around(three, 3)
    four = around(four, 4)
    two, one, own = pair_sums(
        ((0, 0, 2, 0), (0, 1, 2, 1), (1, 0, 1, 0), (1, 1, 1, 1), (2, None, 0, None)),
        (both, both, strip_shape),
        grads,
        theirs,
        where,
    )
    two = around(two, 2)
    one = around(one, 1)
    other = call(add_other, strip_shape, [one, two, three, where], scalars=1)
    other = swap(other)
    strip = call(
        add_replicas,
        shape((32, 16, 1024)),
        [own, one, two, three, four, other, where],
        scalars=1,
    )

    pieces = pl.pallas_call(
        spread_roots,
        out_shape=shape((32, 2, 2, 16, 128)),
        in_specs=[pl.BlockSpec(memory_space=pltpu.HBM)] * 2,
        out_specs=VM,
        scratch_shapes=[
            pltpu.VMEM(left_root.shape, BF),
            pltpu.VMEM(left_root.shape, BF),
            pltpu.SemaphoreType.DMA((2,)),
        ],
        cost_estimate=pl.CostEstimate(flops=1000000, bytes_accessed=524288, transcendentals=0),
    )(left_root, right_root)
    pieces = exchange(pieces, BANDS).reshape(64, 2, 16, 128)
    picked = call(pick_roots, shape((32, 2, 16, 128)), [pieces, table], scalars=1)
    picked = exchange(picked, BANDS)
    left_rows, right_rows = call(join_roots, (shape((4, 16, 1024)), shape((4, 16, 1024))), [picked])

    mine = exchange(strip, ("z", "yl")).reshape(8, 4, 16, 1024)
    other = swap(mine)
    gram, mixed = call(
        products,
        (shape((32, 2, 16, 128)), shape((64, 1024))),
        [mine, other, left_rows, where],
        scalars=1,
        scratch=[pltpu.VMEM((1024, 1024), BF), pltpu.VMEM((128, 1024), BF)],
        flops=2 * 256 * 1024 * 1024,
    )

    gram = exchange(gram, BANDS)
    gram = call(to_slots, shape((32, 2, 2, 16, 128)), [gram, holder], scalars=1)
    gram = exchange(gram, BANDS)
    left_new, right_new = call(
        finish_grams,
        (shape(left_state.shape, F32), shape(right_state.shape, F32)),
        [gram, left_state, right_state],
    )

    theirs = swap(right_rows)
    pair = call(
        pair_up, shape((2, 4, 16, 1024)), [right_rows, theirs, where], scalars=1
    )
    second = around(pair, -2)
    first = around(pair, -1)
    half = call(take_parity, shape((4, 16, 1024)), [second, where], scalars=1)
    third = around(second, -1)
    last = around(half, -2)
    right_mine = call(stack_rows, shape((7, 4, 16, 1024)), [first, second, third, last])
    right_other = swap(right_mine)
    result = call(
        right_product,
        (shape((16, 1024)),) * 4,
        [pair, right_mine, right_other, mixed, where],
        scalars=1,
        scratch=[pltpu.VMEM((1024, 1024), BF), pltpu.VMEM((4, 16, 1024), BF)],
        flops=2 * 64 * 1024 * 1024,
    )
    home = [result[0]] + [shift(result[k], "yl", k) for k in range(1, 4)]
    direction = call(join_columns, shape((1, 1, 16, 4096)), [*home, where], scalars=1)
    return direction, left_new, right_new


def solution(mesh):
    fine = Mesh(mesh.devices.reshape(8, 2, 4, 2, 4), ROWS + BANDS)
    state = P(BANDS, None, ROWS, None, None)
    return jax.shard_map(
        step,
        mesh=fine,
        in_specs=(P(ROWS, BANDS, None), P(), state, state, state, state),
        out_specs=(P(BANDS, ROWS, None, None), state, state),
        check_vma=False,
    )
```
